256 devices in a mesh: grp: 4 (over x), hold: 64 (over y, z, core).
Axes of the slice: x: 4, y: 4, z: 8, core: 2. Of those that a mesh axis runs over, the one named last changes fastest.
Arguments:
- queries: bfloat16 [256, 4096], P(('grp', 'hold')), may hold values from -60 to 60
- prefix_len: int32 [256], P(('grp', 'hold')), may hold values from 128 to 65536
- prefix_keys: bfloat16 [512, 128, 2048], P(('grp', 'hold')), may hold values from -15 to 15
- prefix_values: bfloat16 [512, 128, 2048], P(('grp', 'hold')), may hold values from -24 to 24
- block_table: int32 [512], P(('grp', 'hold')), may hold values from 0 to 511, each once
- suffix_keys: bfloat16 [256, 128, 2048], P(('grp', 'hold')), may hold values from -15 to 15
- suffix_values: bfloat16 [256, 128, 2048], P(('grp', 'hold')), may hold values from -24 to 24
Outputs:
- attention: bfloat16 [256, 4096], P(('grp', 'hold'))
- log_normalizer: float32 [256, 32], P(('grp', 'hold'))
The draws below stay inside these ranges and needn't reach their ends.
All inputs are finite; a program needn't handle non-finite values.
Results may differ from the reference program's by a relative error of at most 0.0035.
Values may be sent and summed in bfloat16 or wider, within the bound.
A program may use at most 64 MiB of HBM per device.

```python
import jax
import jax.numpy as jnp
from jax import lax

HEADS = 32
KV_HEADS = 16
HEAD_DIM = 128
BLOCK = 128
SUFFIX = 128
BLOCKS = 512
PREFIX = 65536
REQUESTS = 256


def joint_draw(key):
    base = jax.random.fold_in(key, 11)
    key_query, key_keys = jax.random.split(base, 2)
    keys = jnp.clip(jax.random.normal(key_keys, (REQUESTS, SUFFIX, KV_HEADS, HEAD_DIM), jnp.float32), -6.0, 6.0) * 2.5
    query = jnp.clip(jax.random.normal(key_query, (REQUESTS, HEADS, HEAD_DIM), jnp.float32), -6.0, 6.0)
    return (query.reshape(REQUESTS, HEADS * HEAD_DIM), keys.reshape(REQUESTS, SUFFIX, KV_HEADS * HEAD_DIM))


def draw_queries(key, part):
    return joint_draw(key)[0].astype(jnp.bfloat16)


def draw_suffix_keys(key, part):
    return joint_draw(key)[1].astype(jnp.bfloat16)


def draw_prefix_keys(key, part):
    base = jax.random.fold_in(key, 31)
    keys = jnp.clip(jax.random.normal(base, (BLOCKS, BLOCK, KV_HEADS, HEAD_DIM), jnp.float32), -6.0, 6.0) * 2.5
    return keys.reshape(BLOCKS, BLOCK, KV_HEADS * HEAD_DIM).astype(jnp.bfloat16)


def touch_ends(array, key, low, high):
    longest = array.shape.index(max(array.shape))
    spots = []
    for shift in (0, 1):
        where = [jax.random.randint(jax.random.fold_in(key, axis), (), 0, length) for axis, length in enumerate(array.shape)]
        where[longest] = (where[longest] + shift) % array.shape[longest]
        spots.append(tuple(where))
    return array.at[spots[0]].set(low).at[spots[1]].set(high)


def levels(stream_key, extent, shards, least, high):
    level, own = 1.0, jax.random.fold_in(stream_key, 6)
    for dim, blocks in shards:
        heights = jnp.exp(jax.random.uniform(jax.random.fold_in(own, dim), (blocks,), jnp.float32, least / len(shards), high / len(shards)))
        level = level * jnp.repeat(heights, extent[dim] // blocks).reshape([-1 if axis == dim else 1 for axis in range(len(extent))])
    return level


def bell_draw(stream_key, shape, spread, reach, cuts=(), kind=jnp.bfloat16):
    result = jax.random.normal(stream_key, shape, jnp.float32) * spread
    if len(cuts) > 0:
        result = levels(stream_key, shape, cuts, -0.22, 0.18) * result
    return jnp.clip(result, min=-reach, max=reach).astype(kind)


def setup_inputs(seed: int = 0) -> dict:
    key_of = jax.random.split(jax.random.key(seed), 8)
    return {
        "queries": draw_queries(jax.random.fold_in(key_of[7], 71), 0),
        "prefix_len": touch_ends(jax.random.randint(key_of[1], (REQUESTS,), BLOCK, PREFIX + 1), jax.random.fold_in(key_of[1], 1), BLOCK, PREFIX).astype(jnp.int32),
        "prefix_keys": draw_prefix_keys(jax.random.fold_in(key_of[7], 71), 0),
        "prefix_values": bell_draw(key_of[3], (BLOCKS, BLOCK, KV_HEADS * HEAD_DIM), 4.0, 24.0, ((0, 256),)),
        "block_table": jax.random.permutation(key_of[4], BLOCKS).astype(jnp.int32),
        "suffix_keys": draw_suffix_keys(jax.random.fold_in(key_of[7], 71), 0),
        "suffix_values": bell_draw(key_of[6], (REQUESTS, SUFFIX, KV_HEADS * HEAD_DIM), 4.0, 24.0, ((0, 256),)),
    }


score_scale = 1.0 / 168.0 ** 0.5
masked_score = -1.0e30


def block_terms(query_heads, keys_heads, values_heads, live, score_form, output_form):
    scores = jnp.einsum(score_form, query_heads, keys_heads) * score_scale
    alive = live[:, None, None, :]
    scores = jnp.where(alive, scores, masked_score)
    block_max = jnp.max(scores, axis=-1)
    weights = jnp.where(alive, jnp.exp(scores - block_max[..., None]), 0.0)
    weights = lax.optimization_barrier(weights.astype(jnp.bfloat16)).astype(jnp.float32)
    block_sum = jnp.sum(weights, axis=-1)
    block_out = jnp.einsum(output_form, weights, values_heads)
    return block_max, block_sum, block_out


def combine_parts(first, second):
    top = jnp.maximum(first[0], second[0])
    left = jnp.exp(first[0] - top)
    right = jnp.exp(second[0] - top)
    return top, first[1] * left + second[1] * right, first[2] * left[..., None] + second[2] * right[..., None]


def reference(queries, prefix_len, prefix_keys, prefix_values, block_table, suffix_keys, suffix_values):
    count = queries.shape[0]
    group = HEADS // KV_HEADS
    query_heads = queries.astype(jnp.float32).reshape(count, KV_HEADS, group, HEAD_DIM)
    suffix_heads = suffix_keys.astype(jnp.float32).reshape(count, SUFFIX, KV_HEADS, HEAD_DIM)
    suffix_vheads = suffix_values.astype(jnp.float32).reshape(count, SUFFIX, KV_HEADS, HEAD_DIM)
    everyone = jnp.zeros((count, SUFFIX), jnp.int32) == 0
    state = block_terms(query_heads, suffix_heads, suffix_vheads, everyone, "rgqd,rtgd->rgqt", "rgqt,rtgd->rgqd")
    offsets = jnp.arange(BLOCK, dtype=jnp.int32)

    def visit(carry, slot):
        keys_slot, values_slot, logical = slot
        keys_heads = keys_slot.astype(jnp.float32).reshape(BLOCK, KV_HEADS, HEAD_DIM)
        values_heads = values_slot.astype(jnp.float32).reshape(BLOCK, KV_HEADS, HEAD_DIM)
        positions = logical * BLOCK + offsets
        live = positions[None, :] < prefix_len[:, None]
        terms = block_terms(query_heads, keys_heads, values_heads, live, "rgqd,tgd->rgqt", "rgqt,tgd->rgqd")
        return combine_parts(carry, terms), None

    state, _ = lax.scan(visit, state, (prefix_keys, prefix_values, block_table))
    top, normalizer, numerator = state
    attention = (numerator / normalizer[..., None]).reshape(count, HEADS * HEAD_DIM).astype(jnp.bfloat16)
    log_normalizer = (top + jnp.log(normalizer)).reshape(count, HEADS)
    return attention, log_normalizer
```

```python
import functools
import math

import jax
import jax.numpy as jnp
from jax import lax
from jax.experimental import pallas as pl
from jax.experimental.pallas import tpu as pltpu
from jax.sharding import Mesh
from jax.sharding import PartitionSpec as P

HEADS = 32
KV_HEADS = 16
HEAD_DIM = 128
HALF = HEADS // 2
KV_HALF = KV_HEADS // 2
AXES = ("x", "y", "z", "c")
MESH = pl.DeviceIdType.MESH

SCALE2 = math.log2(math.e) / 168.0**0.5
LN2 = math.log(2.0)
MASKED = -1e30
FLOOR = -1e29

NT = (((1,), (1,)), ((), ()))
NN = (((1,), (0,)), ((), ()))


def kernel(
    q_ref, len_ref, pos_ref, k_ref, v_ref, ks_ref, vs_ref,
    out_ref, log_ref,
    zq, zl, turn, turn2, qg, kbuf, vbuf, pbuf, ksb, vsb,
    osend, msend, orecv, mrecv, osend2, msend2, orecv2, mrecv2, so, sm, sl,
    local_sem, kv_send, kv_recv, zq_send, zq_recv, zl_send, zl_recv,
    xy_send, xy_recv, ro_send, ro_recv, rm_send, rm_recv,
    fo_send, fo_recv, fm_send, fm_recv,
):
    nx, ny, nz = (lax.axis_size(a) for a in AXES[:3])
    x, y, z, c = (lax.axis_index(a) for a in AXES)
    rows = nz * 2
    mine, plane = z * 2 + c, x * ny + y
    other = 1 - c
    width = KV_HALF * HEAD_DIM

    def columns(half):
        return pl.ds(pl.multiple_of(half * width, width), width)

    loads = [
        pltpu.make_async_copy(k_ref.at[:, :, columns(c)], kbuf.at[0], local_sem.at[0]),
        pltpu.make_async_copy(v_ref.at[:, :, columns(c)], vbuf.at[0], local_sem.at[1]),
        pltpu.make_async_copy(ks_ref, ksb, local_sem.at[2]),
        pltpu.make_async_copy(vs_ref, vsb, local_sem.at[3]),
    ]
    for load in loads:
        load.start()

    line = [(dz, dc) for dz in range(nz) for dc in range(2) if (dz, dc) != (0, 0)]
    sheet = [(dx, dy) for dx in range(nx) for dy in range(ny) if (dx, dy) != (0, 0)]

    def line_id(dz, dc):
        return {"z": lax.rem(z + dz, nz), "c": lax.rem(c + dc, 2)}

    def sheet_id(dx, dy):
        return {"x": lax.rem(x + dx, nx), "y": lax.rem(y + dy, ny)}

    barrier = pltpu.get_barrier_semaphore()
    for dz, dc in line:
        pl.semaphore_signal(barrier, inc=1, device_id=line_id(dz, dc), device_id_type=MESH)
    for dx, dy in sheet:
        pl.semaphore_signal(barrier, inc=1, device_id=sheet_id(dx, dy), device_id_type=MESH)
    pl.semaphore_wait(barrier, len(line) + len(sheet))

    def remote(src, dst, send, recv, device):
        return pltpu.make_async_remote_copy(
            src_ref=src, dst_ref=dst, send_sem=send, recv_sem=recv, device_id=device, device_id_type=MESH
        )

    def line_slot(dz, dc):
        return lax.rem(z + nz - dz, nz) * 2 + lax.rem(c + dc, 2)

    def line_gather(dz, dc, slot):
        i, half = dz * 2 + dc, lax.rem(c + dc, 2)
        device = line_id(dz, dc)
        return [
            remote(q_ref.at[half], zq.at[slot], zq_send.at[i], zq_recv.at[i], device),
            remote(len_ref, zl.at[slot], zl_send.at[i], zl_recv.at[i], device),
        ]

    for dz, dc in line:
        for copy in line_gather(dz, dc, mine):
            copy.start()
    partner = {"c": other}
    swaps = [
        remote(pos_ref, pbuf.at[1], kv_send.at[0], kv_recv.at[0], partner),
        remote(k_ref.at[:, :, columns(other)], kbuf.at[1], kv_send.at[1], kv_recv.at[1], partner),
        remote(v_ref.at[:, :, columns(other)], vbuf.at[1], kv_send.at[2], kv_recv.at[2], partner),
    ]
    for copy in swaps:
        copy.start()
    pbuf[0] = pos_ref[...]
    zq[pl.ds(mine, 1)] = q_ref[pl.ds(c, 1)]
    zl[pl.ds(mine, 1)] = len_ref[...][None]

    loads[2].wait()
    loads[3].wait()
    query = q_ref[...].astype(jnp.float32).reshape(HEADS, HEAD_DIM)
    head_kv = lax.broadcasted_iota(jnp.int32, (HEADS, HEAD_DIM), 0) // 2
    own_scores = jnp.zeros((HEADS, 128), jnp.float32)
    for kv in range(KV_HEADS):
        picked = jnp.where(head_kv == kv, query, 0.0).astype(jnp.bfloat16)
        own_scores += lax.dot_general(
            picked, ksb[0, :, kv * HEAD_DIM : (kv + 1) * HEAD_DIM], NT, preferred_element_type=jnp.float32
        )
    own_scores = own_scores * SCALE2
    own_max = jnp.max(own_scores, axis=1, keepdims=True)
    own_weights = jnp.exp2(own_scores - own_max).astype(jnp.bfloat16)
    own_sum = jnp.sum(own_weights.astype(jnp.float32), axis=1, keepdims=True)
    own_out = jnp.zeros((HEADS, HEAD_DIM), jnp.float32)
    for kv in range(KV_HEADS):
        part = lax.dot_general(
            own_weights, vsb[0, :, kv * HEAD_DIM : (kv + 1) * HEAD_DIM], NN, preferred_element_type=jnp.float32
        )
        own_out += jnp.where(head_kv == kv, part, 0.0)
    so[...] = own_out
    sm[...] = jnp.broadcast_to(own_max, (HEADS, 128))
    sl[...] = jnp.broadcast_to(own_sum, (HEADS, 128))

    for dz, dc in line:
        for copy in line_gather(dz, dc, line_slot(dz, dc)):
            copy.wait_recv()
    turn[...] = zq[...].astype(jnp.float32)
    for h in range(HALF):
        qg[pl.ds(plane, 1), h] = turn[:, h, :].astype(jnp.bfloat16)[None]
    length = zl[:, 0, :]
    high = jnp.floor(length * (1.0 / 256.0))
    lane = lax.broadcasted_iota(jnp.int32, (rows, 128), 1)
    qg[pl.ds(plane, 1), HALF] = jnp.where(lane < 64, high, length - high * 256.0).astype(jnp.bfloat16)[None]

    def sheet_gather(i, device, slot):
        return remote(qg.at[plane], qg.at[slot], xy_send.at[i], xy_recv.at[i], device)

    for dx, dy in sheet:
        sheet_gather(dx * ny + dy, sheet_id(dx, dy), plane).start()

    loads[0].wait()
    loads[1].wait()
    for copy in swaps:
        copy.wait_recv()
    positions = jnp.concatenate([pbuf[s, b : b + 1, :] for s in range(2) for b in range(2)], axis=1)
    tokens = 4 * 128
    ones = jnp.ones((tokens, HEAD_DIM), jnp.bfloat16)
    group = ny * 2 * rows

    def sheet_return(i, device, here, there):
        return [
            remote(osend.at[here], orecv.at[there], ro_send.at[i], ro_recv.at[i], device),
            remote(msend.at[here], mrecv.at[there], rm_send.at[i], rm_recv.at[i], device),
        ]

    def chunk(k, carry):
        column = lax.rem(x + k, nx)
        for dy in range(ny):
            row = lax.rem(y + dy, ny)
            back = lax.rem(nx - k, nx) * ny + (ny - dy) % ny

            def arrive(back=back, row=row):
                sheet_gather(back, {"x": column, "y": row}, column * ny + row).wait_recv()

            if dy == 0:
                pl.when(k > 0)(arrive)
            else:
                arrive()
        base = column * ny
        tile = qg[pl.ds(base, ny), HALF].astype(jnp.float32)
        wide = tile[:, :, 0:1] * 256.0 + tile[:, :, 64:65]
        limit = jnp.broadcast_to(wide[:, None], (ny, 2, rows, 1)).reshape(group, 1)
        live = positions < limit
        lanes = lax.broadcasted_iota(jnp.int32, (ny, rows, 128), 2)
        stats = jnp.zeros((ny, rows, 128), jnp.float32)
        for g in range(KV_HALF):
            span = slice(g * HEAD_DIM, (g + 1) * HEAD_DIM)
            queries = qg[pl.ds(base, ny), 2 * g : 2 * g + 2].reshape(group, HEAD_DIM)
            keys = kbuf[:, :, :, span].reshape(tokens, HEAD_DIM)
            values = vbuf[:, :, :, span].reshape(tokens, HEAD_DIM)
            scores = lax.dot_general(queries, keys, NT, preferred_element_type=jnp.float32) * SCALE2
            scores = jnp.where(live, scores, MASKED)
            top = jnp.maximum(jnp.max(scores, axis=1, keepdims=True), FLOOR)
            weights = jnp.exp2(scores - top).astype(jnp.bfloat16)
            both = lax.dot_general(
                weights, jnp.concatenate([values, ones], axis=1), NN, preferred_element_type=jnp.float32
            )
            osend[pl.ds(base, ny), 2 * g : 2 * g + 2] = (
                both[:, :HEAD_DIM].astype(jnp.bfloat16).reshape(ny, 2, rows, HEAD_DIM)
            )
            tops = jnp.broadcast_to(top, (group, 128)).reshape(ny, 2, rows, 128)
            sums = both[:, HEAD_DIM:].reshape(ny, 2, rows, 128)
            for j in range(2):
                stats = jnp.where(lanes == 2 * g + j, tops[:, j], stats)
                stats = jnp.where(lanes == HALF + 2 * g + j, sums[:, j], stats)
        msend[pl.ds(base, ny)] = stats
        for dy in range(ny):
            row = lax.rem(y + dy, ny)
            there = column * ny + row

            def leave(dy=dy, row=row, there=there):
                for copy in sheet_return(k * ny + dy, {"x": column, "y": row}, there, plane):
                    copy.start()

            if dy == 0:
                pl.when(k > 0)(leave)
            else:
                leave()
        return carry

    lax.fori_loop(0, nx, chunk, 0)

    orecv[pl.ds(plane, 1)] = osend[pl.ds(plane, 1)]
    mrecv[pl.ds(plane, 1)] = msend[pl.ds(plane, 1)]
    for dx, dy in sheet:
        slot = lax.rem(x + nx - dx, nx) * ny + lax.rem(y + ny - dy, ny)
        for copy in sheet_return(dx * ny + dy, sheet_id(dx, dy), slot, slot):
            copy.wait_recv()
    count = nx * ny
    best = jnp.max(mrecv[...], axis=0)

    def merge(s, carry):
        total, out = carry
        part = mrecv[pl.ds(s, 1)][0]
        factor = jnp.exp2(part - best)
        total = total + pltpu.roll(factor, HALF, 1) * part
        block = orecv[pl.ds(s, 1)][0].astype(jnp.float32)
        out = tuple(out[h] + factor[:, h : h + 1] * block[h] for h in range(HALF))
        return total, out

    zero = jnp.zeros((rows, HEAD_DIM), jnp.float32)
    total, out = lax.fori_loop(0, count, merge, (zero, (zero,) * HALF))
    msend2[:, 0, :] = jnp.where(lane < HALF, best, total)
    for h in range(HALF):
        turn2[h] = out[h]
    for r in range(rows):
        osend2[r] = turn2[:, r, :].astype(jnp.bfloat16)

    def line_return(dz, dc, here, there):
        i = dz * 2 + dc
        device = line_id(dz, dc)
        return [
            remote(osend2.at[here], orecv2.at[there], fo_send.at[i], fo_recv.at[i], device),
            remote(msend2.at[here], mrecv2.at[there], fm_send.at[i], fm_recv.at[i], device),
        ]

    for dz, dc in line:
        target = lax.rem(z + dz, nz) * 2 + lax.rem(c + dc, 2)
        for copy in line_return(dz, dc, target, mine):
            copy.start()
    orecv2[pl.ds(mine, 1)] = osend2[pl.ds(mine, 1)]
    mrecv2[pl.ds(mine, 1)] = msend2[pl.ds(mine, 1)]
    for dz, dc in line:
        slot = line_slot(dz, dc)
        for copy in line_return(dz, dc, slot, slot):
            copy.wait_recv()

    lane_of = lax.broadcasted_iota(jnp.int32, (HALF, 128), 1)
    head_of = lax.broadcasted_iota(jnp.int32, (HALF, 128), 0)
    for half in range(2):
        heads = slice(half * HALF, (half + 1) * HALF)
        tops, sums = [sm[heads, 0:1]], [sl[heads, 0:1]]
        for s in range(nz):
            row = jnp.broadcast_to(mrecv2[s * 2 + half], (HALF, 128))
            tops.append(jnp.sum(jnp.where(lane_of == head_of, row, 0.0), axis=1, keepdims=True))
            sums.append(jnp.sum(jnp.where(lane_of == head_of + HALF, row, 0.0), axis=1, keepdims=True))
        top = functools.reduce(jnp.maximum, tops)
        factors = [jnp.exp2(t - top) for t in tops]
        normalizer = sum(f * s for f, s in zip(factors, sums))
        numerator = factors[0] * so[heads, :]
        for s in range(nz):
            numerator += factors[s + 1] * orecv2[s * 2 + half].astype(jnp.float32)
        out_ref[heads, :] = (numerator / normalizer).astype(jnp.bfloat16)
        log_ref[heads, :] = jnp.broadcast_to(top * LN2 + jnp.log(normalizer), (HALF, 128))

    for copy in swaps:
        copy.wait_send()
    for dz, dc in line:
        target = lax.rem(z + dz, nz) * 2 + lax.rem(c + dc, 2)
        for copy in line_gather(dz, dc, mine) + line_return(dz, dc, target, mine):
            copy.wait_send()
    for dx, dy in sheet:
        i, device = dx * ny + dy, sheet_id(dx, dy)
        there = lax.rem(x + dx, nx) * ny + lax.rem(y + dy, ny)
        sheet_gather(i, device, plane).wait_send()
        for copy in sheet_return(i, device, there, plane):
            copy.wait_send()


def body(nx, ny, nz, queries, prefix_len, prefix_keys, prefix_values, block_table, suffix_keys, suffix_values):
    rows, count = nz * 2, nx * ny
    q = queries.reshape(2, HALF, HEAD_DIM)
    length = jnp.broadcast_to(prefix_len.astype(jnp.float32)[:, None], (1, 128))
    offsets = jnp.arange(128, dtype=jnp.int32)
    position = (block_table[:, None] * 128 + offsets[None, :]).astype(jnp.float32)
    position = jnp.pad(position, ((0, 6), (0, 0)))
    vmem, hbm = pl.BlockSpec(memory_space=pltpu.VMEM), pl.BlockSpec(memory_space=pl.ANY)
    bf16, f32 = jnp.bfloat16, jnp.float32
    dma = pltpu.SemaphoreType.DMA
    out, logs = pl.pallas_call(
        kernel,
        name="decode",
        out_shape=[
            jax.ShapeDtypeStruct((HEADS, HEAD_DIM), bf16),
            jax.ShapeDtypeStruct((HEADS, 128), f32),
        ],
        in_specs=[vmem, vmem, vmem, hbm, hbm, hbm, hbm],
        out_specs=[vmem, vmem],
        scratch_shapes=[
            pltpu.VMEM((rows, HALF, HEAD_DIM), bf16),
            pltpu.VMEM((rows, 1, 128), f32),
            pltpu.VMEM((rows, HALF, HEAD_DIM), f32),
            pltpu.VMEM((HALF, rows, HEAD_DIM), f32),
            pltpu.VMEM((count, HALF + 1, rows, HEAD_DIM), bf16),
            pltpu.VMEM((2, 2, 128, KV_HALF * HEAD_DIM), bf16),
            pltpu.VMEM((2, 2, 128, KV_HALF * HEAD_DIM), bf16),
            pltpu.VMEM((2, 8, 128), f32),
            pltpu.VMEM((1, 128, KV_HEADS * HEAD_DIM), bf16),
            pltpu.VMEM((1, 128, KV_HEADS * HEAD_DIM), bf16),
            pltpu.VMEM((count, HALF, rows, HEAD_DIM), bf16),
            pltpu.VMEM((count, rows, 128), f32),
            pltpu.VMEM((count, HALF, rows, HEAD_DIM), bf16),
            pltpu.VMEM((count, rows, 128), f32),
            pltpu.VMEM((rows, HALF, HEAD_DIM), bf16),
            pltpu.VMEM((rows, 1, 128), f32),
            pltpu.VMEM((rows, HALF, HEAD_DIM), bf16),
            pltpu.VMEM((rows, 1, 128), f32),
            pltpu.VMEM((HEADS, HEAD_DIM), f32),
            pltpu.VMEM((HEADS, 128), f32),
            pltpu.VMEM((HEADS, 128), f32),
            dma((4,)), dma((3,)), dma((3,)),
            dma((rows,)), dma((rows,)), dma((rows,)), dma((rows,)),
            dma((count,)), dma((count,)),
            dma((count,)), dma((count,)), dma((count,)), dma((count,)),
            dma((rows,)), dma((rows,)), dma((rows,)), dma((rows,)),
        ],
        compiler_params=pltpu.CompilerParams(
            collective_id=0, has_side_effects=True, vmem_limit_bytes=48 * 1024 * 1024
        ),
    )(q, length, position, prefix_keys, prefix_values, suffix_keys, suffix_values)
    return out.reshape(1, HEADS * HEAD_DIM), logs[:, 0].reshape(1, HEADS)


def solution(mesh):
    shape = mesh.shape
    nx = shape["grp"]
    nz = 8 if shape["hold"] == 64 else 2
    ny = shape["hold"] // (2 * nz)
    split = Mesh(mesh.devices.reshape(nx, ny, nz, 2), AXES)
    rows = P(AXES, None)
    return jax.shard_map(
        functools.partial(body, nx, ny, nz),
        mesh=split,
        in_specs=(rows, P(AXES), P(AXES, None, None), P(AXES, None, None), P(AXES), P(AXES, None, None), P(AXES, None, None)),
        out_specs=(rows, rows),
        check_vma=False,
    )
```

```python
import functools
import math

import jax
import jax.numpy as jnp
from jax import lax
from jax.experimental import pallas as pl
from jax.experimental.pallas import tpu as pltpu
from jax.sharding import Mesh
from jax.sharding import PartitionSpec as P

HEADS = 32
KV_HEADS = 16
HEAD_DIM = 128
HALF = HEADS // 2
KV_HALF = KV_HEADS // 2
FIRST = HALF // 2
AXES = ("x", "y", "z", "c")
MESH = pl.DeviceIdType.MESH

SCALE2 = math.log2(math.e) / 168.0**0.5
LN2 = math.log(2.0)
MASKED = -1e30
FLOOR = -1e29

NT = (((1,), (1,)), ((), ()))
NN = (((1,), (0,)), ((), ()))


def kernel(
    flat_ref, len_ref, table_ref, k_ref, v_ref, ks_ref, vs_ref,
    out_ref, log_ref,
    q_ref, own_len, zq, zl, turn, turn2, qg, kbuf, vbuf, pbuf, ksb, vsb,
    osend, msend, orecv, mrecv, osend2, msend2, orecv2, mrecv2, so, sm, sl,
    local_sem, kv_send, kv_recv, zq_send, zq_recv, zl_send, zl_recv,
    xy_send, xy_recv, ro_send, ro_recv, rm_send, rm_recv,
    fo_send, fo_recv, fm_send, fm_recv,
):
    nx, ny, nz = (lax.axis_size(a) for a in AXES[:3])
    x, y, z, c = (lax.axis_index(a) for a in AXES)
    rows = nz * 2
    mine, plane = z * 2 + c, x * ny + y
    other = 1 - c
    width = KV_HALF * HEAD_DIM

    def columns(half):
        return pl.ds(pl.multiple_of(half * width, width), width)

    loads = [
        pltpu.make_async_copy(k_ref.at[:, :, columns(c)], kbuf.at[0], local_sem.at[0]),
        pltpu.make_async_copy(v_ref.at[:, :, columns(c)], vbuf.at[0], local_sem.at[1]),
        pltpu.make_async_copy(ks_ref, ksb, local_sem.at[2]),
        pltpu.make_async_copy(vs_ref, vsb, local_sem.at[3]),
    ]
    for load in loads:
        load.start()

    flat = flat_ref[...].astype(jnp.float32)
    for h in range(HEADS):
        turn2[h % HALF, 0:1, :] = flat[:, h * HEAD_DIM : (h + 1) * HEAD_DIM]
        if h % HALF == HALF - 1:
            q_ref[h // HALF] = turn2[:, 0, :].astype(jnp.bfloat16)
    own_len[...] = jnp.full((1, 128), len_ref[0], jnp.int32).astype(jnp.float32)
    offset = lax.broadcasted_iota(jnp.int32, (1, 128), 1)
    for b in range(2):
        pbuf[0, b : b + 1, :] = (table_ref[b] * 128 + offset).astype(jnp.float32)

    line = [(dz, dc) for dz in range(nz) for dc in range(2) if (dz, dc) != (0, 0)]
    sheet = [(dx, dy) for dx in range(nx) for dy in range(ny) if (dx, dy) != (0, 0)]

    def line_id(dz, dc):
        return {"z": lax.rem(z + dz, nz), "c": lax.rem(c + dc, 2)}

    def sheet_id(dx, dy):
        return {"x": lax.rem(x + dx, nx), "y": lax.rem(y + dy, ny)}

    barrier = pltpu.get_barrier_semaphore()
    for dz, dc in line:
        pl.semaphore_signal(barrier, inc=1, device_id=line_id(dz, dc), device_id_type=MESH)
    for dx, dy in sheet:
        pl.semaphore_signal(barrier, inc=1, device_id=sheet_id(dx, dy), device_id_type=MESH)
    pl.semaphore_wait(barrier, len(line) + len(sheet))

    def remote(src, dst, send, recv, device):
        return pltpu.make_async_remote_copy(
            src_ref=src, dst_ref=dst, send_sem=send, recv_sem=recv, device_id=device, device_id_type=MESH
        )

    def line_slot(dz, dc):
        return lax.rem(z + nz - dz, nz) * 2 + lax.rem(c + dc, 2)

    def line_gather(dz, dc, slot):
        i, half = dz * 2 + dc, lax.rem(c + dc, 2)
        device = line_id(dz, dc)
        return [
            remote(q_ref.at[half], zq.at[slot], zq_send.at[i], zq_recv.at[i], device),
            remote(own_len, zl.at[slot], zl_send.at[i], zl_recv.at[i], device),
        ]

    for dz, dc in line:
        for copy in line_gather(dz, dc, mine):
            copy.start()
    partner = {"c": other}
    swaps = [
        remote(pbuf.at[0], pbuf.at[1], kv_send.at[0], kv_recv.at[0], partner),
        remote(k_ref.at[:, :, columns(other)], kbuf.at[1], kv_send.at[1], kv_recv.at[1], partner),
        remote(v_ref.at[:, :, columns(other)], vbuf.at[1], kv_send.at[2], kv_recv.at[2], partner),
    ]
    for copy in swaps:
        copy.start()
    zq[pl.ds(mine, 1)] = q_ref[pl.ds(c, 1)]
    zl[pl.ds(mine, 1)] = own_len[...][None]

    loads[2].wait()
    loads[3].wait()
    query = q_ref[...].astype(jnp.float32).reshape(HEADS, HEAD_DIM)
    head_kv = lax.broadcasted_iota(jnp.int32, (HEADS, HEAD_DIM), 0) // 2
    own_scores = jnp.zeros((HEADS, 128), jnp.float32)
    for kv in range(KV_HEADS):
        picked = jnp.where(head_kv == kv, query, 0.0).astype(jnp.bfloat16)
        own_scores += lax.dot_general(
            picked, ksb[0, :, kv * HEAD_DIM : (kv + 1) * HEAD_DIM], NT, preferred_element_type=jnp.float32
        )
    own_scores = own_scores * SCALE2
    own_max = jnp.max(own_scores, axis=1, keepdims=True)
    own_weights = jnp.exp2(own_scores - own_max).astype(jnp.bfloat16)
    own_sum = jnp.sum(own_weights.astype(jnp.float32), axis=1, keepdims=True)
    own_out = jnp.zeros((HEADS, HEAD_DIM), jnp.float32)
    for kv in range(KV_HEADS):
        part = lax.dot_general(
            own_weights, vsb[0, :, kv * HEAD_DIM : (kv + 1) * HEAD_DIM], NN, preferred_element_type=jnp.float32
        )
        own_out += jnp.where(head_kv == kv, part, 0.0)
    so[...] = own_out
    sm[...] = jnp.broadcast_to(own_max, (HEADS, 128))
    sl[...] = jnp.broadcast_to(own_sum, (HEADS, 128))

    for dz, dc in line:
        for copy in line_gather(dz, dc, line_slot(dz, dc)):
            copy.wait_recv()
    turn[...] = zq[...].astype(jnp.float32)
    for h in range(HALF):
        qg[pl.ds(plane, 1), h] = turn[:, h, :].astype(jnp.bfloat16)[None]
    length = zl[:, 0, :]
    high = jnp.floor(length * (1.0 / 256.0))
    lane = lax.broadcasted_iota(jnp.int32, (rows, 128), 1)
    qg[pl.ds(plane, 1), HALF] = jnp.where(lane < 64, high, length - high * 256.0).astype(jnp.bfloat16)[None]

    def sheet_pass(colour, bx, by, dx, dy):
        tiles = pl.ds(0, FIRST) if colour == 0 else pl.ds(FIRST, HALF + 1 - FIRST)
        block = lax.rem(x + bx, nx) * ny + lax.rem(y + by, ny)
        seen = lax.rem(bx + nx - dx, nx) * ny + lax.rem(by + ny - dy, ny)
        sent = (bx + dx) * ny + dy if colour == 0 else dx * ny + by + dy
        return remote(
            qg.at[block, tiles], qg.at[block, tiles],
            xy_send.at[colour, sent], xy_recv.at[colour, seen], sheet_id(dx, dy),
        )

    def sheet_arrival(colour, bx, by):
        tiles = pl.ds(0, FIRST) if colour == 0 else pl.ds(FIRST, HALF + 1 - FIRST)
        block = qg.at[lax.rem(x + bx, nx) * ny + lax.rem(y + by, ny), tiles]
        i = bx * ny + by
        return remote(block, block, xy_send.at[colour, i], xy_recv.at[colour, i], sheet_id(0, 0))

    along_x = [1 + (i // 2 if i % 2 == 0 else nx - 2 - i // 2) for i in range(nx - 1)]
    along_y = [1 + (i // 2 if i % 2 == 0 else ny - 2 - i // 2) for i in range(ny - 1)]
    passes = [(0, 0, 0, dx, 0) for dx in along_x] + [(1, 0, 0, 0, dy) for dy in along_y]
    passes += [(0, 0, 0, 0, dy) for dy in along_y] + [(1, 0, 0, dx, 0) for dx in along_x]
    for step in passes:
        sheet_pass(*step).start()
    seen_first = [(0, bx, 0) for bx in along_x] + [(1, 0, by) for by in along_y]
    for colour, bx, by in sorted(seen_first, key=lambda b: (along_x + along_y).index(b[1] + b[2])):
        sheet_arrival(colour, bx, by).wait_recv()
        onward = [(0, bx, 0, 0, dy) for dy in along_y] if colour == 0 else [(1, 0, by, dx, 0) for dx in along_x]
        for step in onward:
            sheet_pass(*step).start()
        passes += onward

    loads[0].wait()
    loads[1].wait()
    for copy in swaps:
        copy.wait_recv()
    positions = jnp.concatenate([pbuf[s, b : b + 1, :] for s in range(2) for b in range(2)], axis=1)
    tokens = 4 * 128
    ones = jnp.ones((tokens, HEAD_DIM), jnp.bfloat16)
    group = ny * 2 * rows

    def sheet_return(i, device, here, there):
        return [
            remote(osend.at[here], orecv.at[there], ro_send.at[i], ro_recv.at[i], device),
            remote(msend.at[here], mrecv.at[there], rm_send.at[i], rm_recv.at[i], device),
        ]

    def chunk(k, carry):
        column = lax.rem(x + k, nx)
        for dy in range(1, ny):
            sheet_arrival(0, k, dy).wait_recv()

        def arrive():
            for dy in range(ny):
                sheet_arrival(1, k, dy).wait_recv()

        pl.when(k > 0)(arrive)
        base = column * ny
        tile = qg[pl.ds(base, ny), HALF].astype(jnp.float32)
        wide = tile[:, :, 0:1] * 256.0 + tile[:, :, 64:65]
        limit = jnp.broadcast_to(wide[:, None], (ny, 2, rows, 1)).reshape(group, 1)
        live = positions < limit
        lanes = lax.broadcasted_iota(jnp.int32, (ny, rows, 128), 2)
        stats = jnp.zeros((ny, rows, 128), jnp.float32)
        for g in range(KV_HALF):
            span = slice(g * HEAD_DIM, (g + 1) * HEAD_DIM)
            queries = qg[pl.ds(base, ny), 2 * g : 2 * g + 2].reshape(group, HEAD_DIM)
            keys = kbuf[:, :, :, span].reshape(tokens, HEAD_DIM)
            values = vbuf[:, :, :, span].reshape(tokens, HEAD_DIM)
            scores = lax.dot_general(queries, keys, NT, preferred_element_type=jnp.float32) * SCALE2
            scores = jnp.where(live, scores, MASKED)
            top = jnp.maximum(jnp.max(scores, axis=1, keepdims=True), FLOOR)
            weights = jnp.exp2(scores - top).astype(jnp.bfloat16)
            both = lax.dot_general(
                weights, jnp.concatenate([values, ones], axis=1), NN, preferred_element_type=jnp.float32
            )
            osend[pl.ds(base, ny), 2 * g : 2 * g + 2] = (
                both[:, :HEAD_DIM].astype(jnp.bfloat16).reshape(ny, 2, rows, HEAD_DIM)
            )
            tops = jnp.broadcast_to(top, (group, 128)).reshape(ny, 2, rows, 128)
            sums = both[:, HEAD_DIM:].reshape(ny, 2, rows, 128)
            for j in range(2):
                stats = jnp.where(lanes == 2 * g + j, tops[:, j], stats)
                stats = jnp.where(lanes == HALF + 2 * g + j, sums[:, j], stats)
        msend[pl.ds(base, ny)] = stats
        for dy in range(ny):
            row = lax.rem(y + dy, ny)
            there = column * ny + row

            def leave(dy=dy, row=row, there=there):
                for copy in sheet_return(k * ny + dy, {"x": column, "y": row}, there, plane):
                    copy.start()

            if dy == 0:
                pl.when(k > 0)(leave)
            else:
                leave()
        return carry

    lax.fori_loop(0, nx, chunk, 0)

    orecv[pl.ds(plane, 1)] = osend[pl.ds(plane, 1)]
    mrecv[pl.ds(plane, 1)] = msend[pl.ds(plane, 1)]
    for dx, dy in sheet:
        slot = lax.rem(x + nx - dx, nx) * ny + lax.rem(y + ny - dy, ny)
        for copy in sheet_return(dx * ny + dy, sheet_id(dx, dy), slot, slot):
            copy.wait_recv()
    count = nx * ny
    best = jnp.max(mrecv[...], axis=0)

    def merge(s, carry):
        total, out = carry
        part = mrecv[pl.ds(s, 1)][0]
        factor = jnp.exp2(part - best)
        total = total + pltpu.roll(factor, HALF, 1) * part
        block = orecv[pl.ds(s, 1)][0].astype(jnp.float32)
        out = tuple(out[h] + factor[:, h : h + 1] * block[h] for h in range(HALF))
        return total, out

    zero = jnp.zeros((rows, HEAD_DIM), jnp.float32)
    total, out = lax.fori_loop(0, count, merge, (zero, (zero,) * HALF))
    msend2[:, 0, :] = jnp.where(lane < HALF, best, total)
    for h in range(HALF):
        turn2[h] = out[h]
    for r in range(rows):
        osend2[r] = turn2[:, r, :].astype(jnp.bfloat16)

    def line_return(dz, dc, here, there):
        i = dz * 2 + dc
        device = line_id(dz, dc)
        return [
            remote(osend2.at[here], orecv2.at[there], fo_send.at[i], fo_recv.at[i], device),
            remote(msend2.at[here], mrecv2.at[there], fm_send.at[i], fm_recv.at[i], device),
        ]

    for dz, dc in line:
        target = lax.rem(z + dz, nz) * 2 + lax.rem(c + dc, 2)
        for copy in line_return(dz, dc, target, mine):
            copy.start()
    orecv2[pl.ds(mine, 1)] = osend2[pl.ds(mine, 1)]
    mrecv2[pl.ds(mine, 1)] = msend2[pl.ds(mine, 1)]
    for dz, dc in line:
        slot = line_slot(dz, dc)
        for copy in line_return(dz, dc, slot, slot):
            copy.wait_recv()

    lane_of = lax.broadcasted_iota(jnp.int32, (HALF, 128), 1)
    head_of = lax.broadcasted_iota(jnp.int32, (HALF, 128), 0)
    for half in range(2):
        heads = slice(half * HALF, (half + 1) * HALF)
        tops, sums = [sm[heads, 0:1]], [sl[heads, 0:1]]
        for s in range(nz):
            row = jnp.broadcast_to(mrecv2[s * 2 + half], (HALF, 128))
            tops.append(jnp.sum(jnp.where(lane_of == head_of, row, 0.0), axis=1, keepdims=True))
            sums.append(jnp.sum(jnp.where(lane_of == head_of + HALF, row, 0.0), axis=1, keepdims=True))
        top = functools.reduce(jnp.maximum, tops)
        factors = [jnp.exp2(t - top) for t in tops]
        normalizer = sum(f * s for f, s in zip(factors, sums))
        numerator = factors[0] * so[heads, :]
        for s in range(nz):
            numerator += factors[s + 1] * orecv2[s * 2 + half].astype(jnp.float32)
        out_ref[heads, :] = (numerator / normalizer).astype(jnp.bfloat16)
        log_ref[heads, :] = jnp.broadcast_to(top * LN2 + jnp.log(normalizer), (HALF, 128))

    for copy in swaps:
        copy.wait_send()
    for dz, dc in line:
        target = lax.rem(z + dz, nz) * 2 + lax.rem(c + dc, 2)
        for copy in line_gather(dz, dc, mine) + line_return(dz, dc, target, mine):
            copy.wait_send()
    for step in passes:
        sheet_pass(*step).wait_send()
    for dx, dy in sheet:
        i, device = dx * ny + dy, sheet_id(dx, dy)
        there = lax.rem(x + dx, nx) * ny + lax.rem(y + dy, ny)
        for copy in sheet_return(i, device, there, plane):
            copy.wait_send()


def body(nx, ny, nz, queries, prefix_len, prefix_keys, prefix_values, block_table, suffix_keys, suffix_values):
    rows, count = nz * 2, nx * ny
    vmem, smem, hbm = (pl.BlockSpec(memory_space=m) for m in (pltpu.VMEM, pltpu.SMEM, pl.ANY))
    bf16, f32 = jnp.bfloat16, jnp.float32
    dma = pltpu.SemaphoreType.DMA
    out, logs = pl.pallas_call(
        kernel,
        name="decode",
        out_shape=[
            jax.ShapeDtypeStruct((HEADS, HEAD_DIM), bf16),
            jax.ShapeDtypeStruct((HEADS, 128), f32),
        ],
        in_specs=[vmem, smem, smem, hbm, hbm, hbm, hbm],
        out_specs=[vmem, vmem],
        scratch_shapes=[
            pltpu.VMEM((2, HALF, HEAD_DIM), bf16),
            pltpu.VMEM((1, 128), f32),
            pltpu.VMEM((rows, HALF, HEAD_DIM), bf16),
            pltpu.VMEM((rows, 1, 128), f32),
            pltpu.VMEM((rows, HALF, HEAD_DIM), f32),
            pltpu.VMEM((HALF, rows, HEAD_DIM), f32),
            pltpu.VMEM((count, HALF + 1, rows, HEAD_DIM), bf16),
            pltpu.VMEM((2, 2, 128, KV_HALF * HEAD_DIM), bf16),
            pltpu.VMEM((2, 2, 128, KV_HALF * HEAD_DIM), bf16),
            pltpu.VMEM((2, 8, 128), f32),
            pltpu.VMEM((1, 128, KV_HEADS * HEAD_DIM), bf16),
            pltpu.VMEM((1, 128, KV_HEADS * HEAD_DIM), bf16),
            pltpu.VMEM((count, HALF, rows, HEAD_DIM), bf16),
            pltpu.VMEM((count, rows, 128), f32),
            pltpu.VMEM((count, HALF, rows, HEAD_DIM), bf16),
            pltpu.VMEM((count, rows, 128), f32),
            pltpu.VMEM((rows, HALF, HEAD_DIM), bf16),
            pltpu.VMEM((rows, 1, 128), f32),
            pltpu.VMEM((rows, HALF, HEAD_DIM), bf16),
            pltpu.VMEM((rows, 1, 128), f32),
            pltpu.VMEM((HEADS, HEAD_DIM), f32),
            pltpu.VMEM((HEADS, 128), f32),
            pltpu.VMEM((HEADS, 128), f32),
            dma((4,)), dma((3,)), dma((3,)),
            dma((rows,)), dma((rows,)), dma((rows,)), dma((rows,)),
            dma((2, count)), dma((2, count)),
            dma((count,)), dma((count,)), dma((count,)), dma((count,)),
            dma((rows,)), dma((rows,)), dma((rows,)), dma((rows,)),
        ],
        compiler_params=pltpu.CompilerParams(
            collective_id=0, has_side_effects=True, vmem_limit_bytes=63 * 1024 * 1024
        ),
    )(queries, prefix_len, block_table, prefix_keys, prefix_values, suffix_keys, suffix_values)
    return out.reshape(1, HEADS * HEAD_DIM), logs[:, 0].reshape(1, HEADS)


def solution(mesh):
    shape = mesh.shape
    nx = shape["grp"]
    nz = 8 if shape["hold"] == 64 else 2
    ny = shape["hold"] // (2 * nz)
    split = Mesh(mesh.devices.reshape(nx, ny, nz, 2), AXES)
    rows = P(AXES, None)
    return jax.shard_map(
        functools.partial(body, nx, ny, nz),
        mesh=split,
        in_specs=(rows, P(AXES), P(AXES, None, None), P(AXES, None, None), P(AXES), P(AXES, None, None), P(AXES, None, None)),
        out_specs=(rows, rows),
        check_vma=False,
    )
```

```python
import functools
import math

import jax
import jax.numpy as jnp
from jax import lax
from jax.experimental import pallas as pl
from jax.experimental.pallas import tpu as pltpu
from jax.sharding import Mesh
from jax.sharding import PartitionSpec as P

HEADS = 32
KV_HEADS = 16
HEAD_DIM = 128
TYPES = 4
LOCAL = HEADS // TYPES
KV_SET = 2
PAIR = KV_SET * HEAD_DIM
FIRST = LOCAL // 2
AXES = ("x", "y", "z", "c")
MESH = pl.DeviceIdType.MESH

SCALE2 = math.log2(math.e) / 168.0**0.5
LN2 = math.log(2.0)
MASKED = -1e30
FLOOR = -1e29

NT = (((1,), (1,)), ((), ()))
NN = (((1,), (0,)), ((), ()))


def kernel(
    flat_ref, len_ref, table_ref, k_ref, v_ref, ks_ref, vs_ref,
    out_ref, log_ref,
    q_ref, own_len, zq, zl, turn, turn2, qg, kbuf, vbuf, pbuf, ksb, vsb,
    osend, msend, orecv, mrecv, osend2, msend2, orecv2, mrecv2, so, sm, sl, natural,
    local_sem, kv_send, kv_recv, zq_send, zq_recv, zl_send, zl_recv,
    xy_send, xy_recv, ro_send, ro_recv, rm_send, rm_recv,
    fo_send, fo_recv, fm_send, fm_recv,
):
    nx, ny, nz = (lax.axis_size(a) for a in AXES[:3])
    x, y, z, c = (lax.axis_index(a) for a in AXES)
    rows = nz * 2
    mine, plane = z * 2 + c, x * ny + y
    other = 1 - c
    odd = lax.rem(z, 2)
    pairs = [z + 1 - 2 * odd, lax.rem(z + nz - 1 + 2 * odd, nz)]

    def kind(zz, cc):
        return lax.rem(zz, 2) * 2 + cc

    def columns(s, t):
        return pl.ds(pl.multiple_of(s * 8 * HEAD_DIM + t * PAIR, PAIR), PAIR)

    mykind = kind(z, c)
    loads = [
        pltpu.make_async_copy(ks_ref, ksb, local_sem.at[0]),
        pltpu.make_async_copy(vs_ref, vsb, local_sem.at[1]),
    ]
    for s in range(2):
        loads += [
            pltpu.make_async_copy(k_ref.at[:, :, columns(s, mykind)], kbuf.at[s, 0], local_sem.at[2 + s]),
            pltpu.make_async_copy(v_ref.at[:, :, columns(s, mykind)], vbuf.at[s, 0], local_sem.at[4 + s]),
        ]
    for load in loads:
        load.start()

    flat = flat_ref[...].astype(jnp.float32)
    for t in range(TYPES):
        for i in range(LOCAL):
            h = 16 * (i // 4) + 4 * t + i % 4
            turn2[i, 0:1, :] = flat[:, h * HEAD_DIM : (h + 1) * HEAD_DIM]
        q_ref[t] = turn2[:, 0, :].astype(jnp.bfloat16)
    own_len[...] = jnp.full((1, 128), len_ref[0], jnp.int32).astype(jnp.float32)
    offset = lax.broadcasted_iota(jnp.int32, (1, 128), 1)
    for b in range(2):
        pbuf[0, b : b + 1, :] = (table_ref[b] * 128 + offset).astype(jnp.float32)

    line = [(dz, dc) for dz in range(nz) for dc in range(2) if (dz, dc) != (0, 0)]
    sheet = [(dx, dy) for dx in range(nx) for dy in range(ny) if (dx, dy) != (0, 0)]

    def line_id(dz, dc):
        return {"z": lax.rem(z + dz, nz), "c": lax.rem(c + dc, 2)}

    def sheet_id(dx, dy):
        return {"x": lax.rem(x + dx, nx), "y": lax.rem(y + dy, ny)}

    barrier = pltpu.get_barrier_semaphore()
    for dz, dc in line:
        pl.semaphore_signal(barrier, inc=1, device_id=line_id(dz, dc), device_id_type=MESH)
    for dx, dy in sheet:
        pl.semaphore_signal(barrier, inc=1, device_id=sheet_id(dx, dy), device_id_type=MESH)
    pl.semaphore_wait(barrier, len(line) + len(sheet))

    def remote(src, dst, send, recv, device):
        return pltpu.make_async_remote_copy(
            src_ref=src, dst_ref=dst, send_sem=send, recv_sem=recv, device_id=device, device_id_type=MESH
        )

    def line_slot(dz, dc):
        return lax.rem(z + nz - dz, nz) * 2 + lax.rem(c + dc, 2)

    def line_gather(dz, dc, slot):
        i, to = dz * 2 + dc, kind(lax.rem(z + dz, nz), lax.rem(c + dc, 2))
        device = line_id(dz, dc)
        return [
            remote(q_ref.at[to], zq.at[slot], zq_send.at[i], zq_recv.at[i], device),
            remote(own_len, zl.at[slot], zl_send.at[i], zl_recv.at[i], device),
        ]

    for dz, dc in line:
        for copy in line_gather(dz, dc, mine):
            copy.start()
    partner = {"c": other}
    swaps = [remote(pbuf.at[0], pbuf.at[1], kv_send.at[12], kv_recv.at[12], partner)]
    for s in range(2):
        for dc in range(2):
            i, device = 2 * s + dc, {"z": pairs[s], "c": lax.rem(c + dc, 2)}
            swaps.append(remote(pbuf.at[0], pbuf.at[2 + i], kv_send.at[13 + i], kv_recv.at[13 + i], device))
    for ref, buf, at in ((k_ref, kbuf, 0), (v_ref, vbuf, 6)):
        for s in range(2):
            source = ref.at[:, :, columns(s, kind(z, other))]
            swaps.append(remote(source, buf.at[s, 1], kv_send.at[at + s], kv_recv.at[at + s], partner))
            for dc in range(2):
                i, core = at + 2 + 2 * s + dc, lax.rem(c + dc, 2)
                source = ref.at[:, :, columns(s, kind(pairs[s], core))]
                device = {"z": pairs[s], "c": core}
                swaps.append(remote(source, buf.at[s, 2 + dc], kv_send.at[i], kv_recv.at[i], device))
    for copy in swaps:
        copy.start()
    zq[pl.ds(mine, 1)] = q_ref[pl.ds(mykind, 1)]
    zl[pl.ds(mine, 1)] = own_len[...][None]

    loads[0].wait()
    loads[1].wait()
    query = q_ref[...].astype(jnp.float32).reshape(HEADS, HEAD_DIM)
    place = lax.broadcasted_iota(jnp.int32, (HEADS, HEAD_DIM), 0)
    head_kv = place % LOCAL // 4 * 8 + place // LOCAL * 2 + place % 4 // 2
    own_scores = jnp.zeros((HEADS, 128), jnp.float32)
    for kv in range(KV_HEADS):
        picked = jnp.where(head_kv == kv, query, 0.0).astype(jnp.bfloat16)
        own_scores += lax.dot_general(
            picked, ksb[0, :, kv * HEAD_DIM : (kv + 1) * HEAD_DIM], NT, preferred_element_type=jnp.float32
        )
    own_scores = own_scores * SCALE2
    own_max = jnp.max(own_scores, axis=1, keepdims=True)
    own_weights = jnp.exp2(own_scores - own_max).astype(jnp.bfloat16)
    own_sum = jnp.sum(own_weights.astype(jnp.float32), axis=1, keepdims=True)
    own_out = jnp.zeros((HEADS, HEAD_DIM), jnp.float32)
    for kv in range(KV_HEADS):
        part = lax.dot_general(
            own_weights, vsb[0, :, kv * HEAD_DIM : (kv + 1) * HEAD_DIM], NN, preferred_element_type=jnp.float32
        )
        own_out += jnp.where(head_kv == kv, part, 0.0)
    so[...] = own_out
    sm[...] = jnp.broadcast_to(own_max, (HEADS, 128))
    sl[...] = jnp.broadcast_to(own_sum, (HEADS, 128))

    for dz, dc in line:
        for copy in line_gather(dz, dc, line_slot(dz, dc)):
            copy.wait_recv()
    turn[...] = zq[...].astype(jnp.float32)
    for h in range(LOCAL):
        qg[pl.ds(plane, 1), h] = turn[:, h, :].astype(jnp.bfloat16)[None]
    length = zl[:, 0, :]
    high = jnp.floor(length * (1.0 / 256.0))
    lane = lax.broadcasted_iota(jnp.int32, (rows, 128), 1)
    qg[pl.ds(plane, 1), LOCAL] = jnp.where(lane < 64, high, length - high * 256.0).astype(jnp.bfloat16)[None]

    def sheet_pass(colour, bx, by, dx, dy):
        tiles = pl.ds(0, FIRST) if colour == 0 else pl.ds(FIRST, LOCAL + 1 - FIRST)
        block = lax.rem(x + bx, nx) * ny + lax.rem(y + by, ny)
        seen = lax.rem(bx + nx - dx, nx) * ny + lax.rem(by + ny - dy, ny)
        sent = (bx + dx) * ny + dy if colour == 0 else dx * ny + by + dy
        return remote(
            qg.at[block, tiles], qg.at[block, tiles],
            xy_send.at[colour, sent], xy_recv.at[colour, seen], sheet_id(dx, dy),
        )

    def sheet_arrival(colour, bx, by):
        tiles = pl.ds(0, FIRST) if colour == 0 else pl.ds(FIRST, LOCAL + 1 - FIRST)
        block = qg.at[lax.rem(x + bx, nx) * ny + lax.rem(y + by, ny), tiles]
        i = bx * ny + by
        return remote(block, block, xy_send.at[colour, i], xy_recv.at[colour, i], sheet_id(0, 0))

    along_x = [1 + (i // 2 if i % 2 == 0 else nx - 2 - i // 2) for i in range(nx - 1)]
    along_y = [1 + (i // 2 if i % 2 == 0 else ny - 2 - i // 2) for i in range(ny - 1)]
    passes = [(0, 0, 0, dx, 0) for dx in along_x] + [(1, 0, 0, 0, dy) for dy in along_y]
    passes += [(0, 0, 0, 0, dy) for dy in along_y] + [(1, 0, 0, dx, 0) for dx in along_x]
    for step in passes:
        sheet_pass(*step).start()
    seen_first = [(0, bx, 0) for bx in along_x] + [(1, 0, by) for by in along_y]
    for colour, bx, by in sorted(seen_first, key=lambda b: (along_x + along_y).index(b[1] + b[2])):
        sheet_arrival(colour, bx, by).wait_recv()
        onward = [(0, bx, 0, 0, dy) for dy in along_y] if colour == 0 else [(1, 0, by, dx, 0) for dx in along_x]
        for step in onward:
            sheet_pass(*step).start()
        passes += onward

    for load in loads[2:]:
        load.wait()
    for copy in swaps:
        copy.wait_recv()
    tokens = 8 * 128
    positions = [
        jnp.concatenate([pbuf[p, b : b + 1, :] for p in (0, 1, 2 + 2 * s, 3 + 2 * s) for b in range(2)], axis=1)
        for s in range(2)
    ]
    ones = jnp.ones((tokens, HEAD_DIM), jnp.bfloat16)
    group = ny * 2 * rows
    pile = min(rows, 8)

    def packed(tile):
        tile = tile.reshape(-1, pile, 128)
        return jnp.stack([
            jnp.sum(pltpu.roll(tile[i], 0, 1, stride=16, stride_axis=0), axis=0) for i in range(rows // pile)
        ])

    def sheet_return(i, device, here, there):
        return [
            remote(osend.at[here], orecv.at[there], ro_send.at[i], ro_recv.at[i], device),
            remote(msend.at[here], mrecv.at[there], rm_send.at[i], rm_recv.at[i], device),
        ]

    def chunk(k, carry):
        column = lax.rem(x + k, nx)
        for dy in range(1, ny):
            sheet_arrival(0, k, dy).wait_recv()

        def arrive():
            for dy in range(ny):
                sheet_arrival(1, k, dy).wait_recv()

        pl.when(k > 0)(arrive)
        base = column * ny
        tile = qg[pl.ds(base, ny), LOCAL].astype(jnp.float32)
        wide = tile[:, :, 0:1] * 256.0 + tile[:, :, 64:65]
        limit = jnp.broadcast_to(wide[:, None], (ny, 2, rows, 1)).reshape(group, 1)
        live = [position < limit for position in positions]
        lanes = lax.broadcasted_iota(jnp.int32, (ny, rows, 128), 2)
        stats = jnp.zeros((ny, rows, 128), jnp.float32)
        for g in range(2 * KV_SET):
            s, span = g // KV_SET, slice(g % KV_SET * HEAD_DIM, (g % KV_SET + 1) * HEAD_DIM)
            queries = qg[pl.ds(base, ny), 2 * g : 2 * g + 2].reshape(group, HEAD_DIM)
            keys = kbuf[s, :, :, :, span].reshape(tokens, HEAD_DIM)
            values = vbuf[s, :, :, :, span].reshape(tokens, HEAD_DIM)
            scores = lax.dot_general(queries, keys, NT, preferred_element_type=jnp.float32) * SCALE2
            scores = jnp.where(live[s], scores, MASKED)
            top = jnp.maximum(jnp.max(scores, axis=1, keepdims=True), FLOOR)
            weights = jnp.exp2(scores - top).astype(jnp.bfloat16)
            both = lax.dot_general(
                weights, jnp.concatenate([values, ones], axis=1), NN, preferred_element_type=jnp.float32
            )
            osend[pl.ds(base, ny), 2 * g : 2 * g + 2] = (
                both[:, :HEAD_DIM].astype(jnp.bfloat16).reshape(ny, 2, rows, HEAD_DIM)
            )
            tops = jnp.broadcast_to(top, (group, 128)).reshape(ny, 2, rows, 128)
            sums = both[:, HEAD_DIM:].reshape(ny, 2, rows, 128)
            for j in range(2):
                stats = jnp.where(lanes == 2 * g + j, tops[:, j], stats)
                stats = jnp.where(lanes == LOCAL + 2 * g + j, sums[:, j], stats)
        for i in range(ny):
            msend[pl.ds(base + i, 1)] = packed(stats[i])[None]
        for dy in range(ny):
            row = lax.rem(y + dy, ny)
            there = column * ny + row

            def leave(dy=dy, row=row, there=there):
                for copy in sheet_return(k * ny + dy, {"x": column, "y": row}, there, plane):
                    copy.start()

            if dy == 0:
                pl.when(k > 0)(leave)
            else:
                leave()
        return carry

    lax.fori_loop(0, nx, chunk, 0)

    orecv[pl.ds(plane, 1)] = osend[pl.ds(plane, 1)]
    mrecv[pl.ds(plane, 1)] = msend[pl.ds(plane, 1)]
    for dx, dy in sheet:
        slot = lax.rem(x + nx - dx, nx) * ny + lax.rem(y + ny - dy, ny)
        for copy in sheet_return(dx * ny + dy, sheet_id(dx, dy), slot, slot):
            copy.wait_recv()
    count = nx * ny
    best = jnp.max(mrecv[...], axis=0)
    at_row = lax.broadcasted_iota(jnp.int32, (rows, 128), 0) % pile * 16

    def merge(s, carry):
        total, out = carry
        part = mrecv[pl.ds(s, 1)][0]
        factor = jnp.exp2(part - best)
        total = total + pltpu.roll(factor, LOCAL, 1) * part
        spread = jnp.concatenate(
            [jnp.broadcast_to(factor[i : i + 1], (pile, 128)) for i in range(rows // pile)], axis=0
        )
        block = orecv[pl.ds(s, 1)][0].astype(jnp.float32)
        out = tuple(
            out[h] + jnp.sum(jnp.where(lane == at_row + h, spread, 0.0), axis=1, keepdims=True) * block[h]
            for h in range(LOCAL)
        )
        return total, out

    zero = jnp.zeros((rows, HEAD_DIM), jnp.float32)
    total, out = lax.fori_loop(0, count, merge, (jnp.zeros_like(best), (zero,) * LOCAL))
    msend2[...] = jnp.where(lane[: rows // pile] % 16 < LOCAL, best, total)
    for h in range(LOCAL):
        turn2[h] = out[h]
    for r in range(rows):
        osend2[r] = turn2[:, r, :]

    def line_return(dz, dc, here, there):
        i = dz * 2 + dc
        device = line_id(dz, dc)
        return [
            remote(osend2.at[here], orecv2.at[there], fo_send.at[i], fo_recv.at[i], device),
            remote(msend2, mrecv2.at[there], fm_send.at[i], fm_recv.at[i], device),
        ]

    for dz, dc in line:
        target = lax.rem(z + dz, nz) * 2 + lax.rem(c + dc, 2)
        for copy in line_return(dz, dc, target, mine):
            copy.start()
    orecv2[pl.ds(mine, 1)] = osend2[pl.ds(mine, 1)]
    mrecv2[pl.ds(mine, 1)] = msend2[...][None]
    for dz, dc in line:
        slot = line_slot(dz, dc)
        for copy in line_return(dz, dc, slot, slot):
            copy.wait_recv()

    lane_of = lax.broadcasted_iota(jnp.int32, (LOCAL, 128), 1)
    head_of = lax.broadcasted_iota(jnp.int32, (LOCAL, 128), 0)
    pick = lax.rem(mine, pile) * 16 + head_of
    for t in range(TYPES):
        heads = slice(t * LOCAL, (t + 1) * LOCAL)
        slots = [zz * 2 + t % 2 for zz in range(nz) if zz % 2 == t // 2]
        tops, sums = [sm[heads, 0:1]], [sl[heads, 0:1]]
        for slot in slots:
            row = jnp.broadcast_to(mrecv2[slot, pl.ds(mine // pile, 1), :], (LOCAL, 128))
            tops.append(jnp.sum(jnp.where(lane_of == pick, row, 0.0), axis=1, keepdims=True))
            sums.append(jnp.sum(jnp.where(lane_of == pick + LOCAL, row, 0.0), axis=1, keepdims=True))
        top = functools.reduce(jnp.maximum, tops)
        factors = [jnp.exp2(m - top) for m in tops]
        normalizer = sum(f * l for f, l in zip(factors, sums))
        numerator = factors[0] * so[heads, :]
        for f, slot in zip(factors[1:], slots):
            numerator += f * orecv2[slot]
        numerator = numerator / normalizer
        logs = jnp.broadcast_to(top * LN2 + jnp.log(normalizer), (LOCAL, 128))
        for s in range(2):
            there, here = slice(16 * s + 4 * t, 16 * s + 4 * t + 4), slice(4 * s, 4 * s + 4)
            natural[there, :] = numerator[here]
            log_ref[there, :] = logs[here]
    out_ref[...] = natural[...].astype(jnp.bfloat16)

    for copy in swaps:
        copy.wait_send()
    for dz, dc in line:
        target = lax.rem(z + dz, nz) * 2 + lax.rem(c + dc, 2)
        for copy in line_gather(dz, dc, mine) + line_return(dz, dc, target, mine):
            copy.wait_send()
    for step in passes:
        sheet_pass(*step).wait_send()
    for dx, dy in sheet:
        i, device = dx * ny + dy, sheet_id(dx, dy)
        there = lax.rem(x + dx, nx) * ny + lax.rem(y + dy, ny)
        for copy in sheet_return(i, device, there, plane):
            copy.wait_send()


def body(nx, ny, nz, queries, prefix_len, prefix_keys, prefix_values, block_table, suffix_keys, suffix_values):
    rows, count = nz * 2, nx * ny
    piles = rows // min(rows, 8)
    vmem, smem, hbm = (pl.BlockSpec(memory_space=m) for m in (pltpu.VMEM, pltpu.SMEM, pl.ANY))
    bf16, f32 = jnp.bfloat16, jnp.float32
    dma = pltpu.SemaphoreType.DMA
    out, logs = pl.pallas_call(
        kernel,
        name="decode",
        out_shape=[
            jax.ShapeDtypeStruct((HEADS, HEAD_DIM), bf16),
            jax.ShapeDtypeStruct((HEADS, 128), f32),
        ],
        in_specs=[vmem, smem, smem, hbm, hbm, hbm, hbm],
        out_specs=[vmem, vmem],
        scratch_shapes=[
            pltpu.VMEM((TYPES, LOCAL, HEAD_DIM), bf16),
            pltpu.VMEM((1, 128), f32),
            pltpu.VMEM((rows, LOCAL, HEAD_DIM), bf16),
            pltpu.VMEM((rows, 1, 128), f32),
            pltpu.VMEM((rows, LOCAL, HEAD_DIM), f32),
            pltpu.VMEM((LOCAL, rows, HEAD_DIM), f32),
            pltpu.VMEM((count, LOCAL + 1, rows, HEAD_DIM), bf16),
            pltpu.VMEM((2, 4, 2, 128, PAIR), bf16),
            pltpu.VMEM((2, 4, 2, 128, PAIR), bf16),
            pltpu.VMEM((6, 8, 128), f32),
            pltpu.VMEM((1, 128, KV_HEADS * HEAD_DIM), bf16),
            pltpu.VMEM((1, 128, KV_HEADS * HEAD_DIM), bf16),
            pltpu.VMEM((count, LOCAL, rows, HEAD_DIM), bf16),
            pltpu.VMEM((count, piles, 128), f32),
            pltpu.VMEM((count, LOCAL, rows, HEAD_DIM), bf16),
            pltpu.VMEM((count, piles, 128), f32),
            pltpu.VMEM((rows, LOCAL, HEAD_DIM), f32),
            pltpu.VMEM((piles, 128), f32),
            pltpu.VMEM((rows, LOCAL, HEAD_DIM), f32),
            pltpu.VMEM((rows, piles, 128), f32),
            pltpu.VMEM((HEADS, HEAD_DIM), f32),
            pltpu.VMEM((HEADS, 128), f32),
            pltpu.VMEM((HEADS, 128), f32),
            pltpu.VMEM((HEADS, HEAD_DIM), f32),
            dma((6,)), dma((17,)), dma((17,)),
            dma((rows,)), dma((rows,)), dma((rows,)), dma((rows,)),
            dma((2, count)), dma((2, count)),
            dma((count,)), dma((count,)), dma((count,)), dma((count,)),
            dma((rows,)), dma((rows,)), dma((rows,)), dma((rows,)),
        ],
        compiler_params=pltpu.CompilerParams(
            collective_id=0, has_side_effects=True, vmem_limit_bytes=63 * 1024 * 1024
        ),
    )(queries, prefix_len, block_table, prefix_keys, prefix_values, suffix_keys, suffix_values)
    return out.reshape(1, HEADS * HEAD_DIM), logs[:, 0].reshape(1, HEADS)


def sizes(mesh):
    nx = mesh.shape["grp"]
    nz = 8 if mesh.shape["hold"] == 64 else 2
    return nx, mesh.shape["hold"] // (2 * nz), nz


def solution(mesh):
    nx, ny, nz = sizes(mesh)
    split = Mesh(mesh.devices.reshape(nx, ny, nz, 2), AXES)
    rows = P(AXES, None)
    return jax.shard_map(
        functools.partial(body, nx, ny, nz),
        mesh=split,
        in_specs=(rows, P(AXES), P(AXES, None, None), P(AXES, None, None), P(AXES), P(AXES, None, None), P(AXES, None, None)),
        out_specs=(rows, rows),
        check_vma=False,
    )
```

```python
import functools
import math

import jax
import jax.numpy as jnp
from jax import lax
from jax.experimental import pallas as pl
from jax.experimental.pallas import tpu as pltpu
from jax.sharding import Mesh
from jax.sharding import PartitionSpec as P

HEADS = 32
KV_HEADS = 16
HEAD_DIM = 128
TYPES = 4
LOCAL = HEADS // TYPES
FIRST = LOCAL // 2
AXES = ("x", "y", "z", "c")
MESH = pl.DeviceIdType.MESH

SCALE2 = math.log2(math.e) / 168.0**0.5
LN2 = math.log(2.0)
MASKED = -1e30
FLOOR = -1e29

NT = (((1,), (1,)), ((), ()))
NN = (((1,), (0,)), ((), ()))


def kernel(
    flat_hbm, len_hbm, table_hbm, k_ref, v_ref, ks_ref, vs_ref,
    out_ref, log_ref,
    flat_ref, len_ref, table_ref, q_ref, own_len, zq, zl, turn, turn2, qg, kbuf, vbuf, pbuf, ksb, vsb,
    osend, msend, orecv, mrecv, osend2, msend2, orecv2, mrecv2, so, sm, sl, natural,
    small_sem, local_sem, kv_send, kv_recv, zq_send, zq_recv, zl_send, zl_recv,
    xy_send, xy_recv, ro_send, ro_recv, rm_send, rm_recv,
    fo_send, fo_recv, fm_send, fm_recv,
):
    nx, ny, nz = (lax.axis_size(a) for a in AXES[:3])
    x, y, z, c = (lax.axis_index(a) for a in AXES)
    rows = nz * 2
    mine, plane = z * 2 + c, x * ny + y
    other = 1 - c
    odd = lax.rem(z, 2)
    pairs = [z + 1 - 2 * odd, lax.rem(z + nz - 1 + 2 * odd, nz)]

    def kind(zz, cc):
        return lax.rem(zz, 2) * 2 + cc

    def columns(s, t, e):
        return pl.ds(pl.multiple_of((s * 8 + t * 2 + e) * HEAD_DIM, HEAD_DIM), HEAD_DIM)

    small = [
        pltpu.make_async_copy(src, dst, small_sem.at[i])
        for i, (src, dst) in enumerate([(flat_hbm, flat_ref), (len_hbm, len_ref), (table_hbm, table_ref)])
    ]
    for copy in small:
        copy.start()
    line = [(dz, dc) for dz in range(nz) for dc in range(2) if (dz, dc) != (0, 0)]
    sheet = [(dx, dy) for dx in range(nx) for dy in range(ny) if (dx, dy) != (0, 0)]

    def line_id(dz, dc):
        return {"z": lax.rem(z + dz, nz), "c": lax.rem(c + dc, 2)}

    def sheet_id(dx, dy):
        return {"x": lax.rem(x + dx, nx), "y": lax.rem(y + dy, ny)}

    barrier = pltpu.get_barrier_semaphore()
    for dz, dc in line:
        pl.semaphore_signal(barrier, inc=1, device_id=line_id(dz, dc), device_id_type=MESH)
    for dx, dy in sheet:
        pl.semaphore_signal(barrier, inc=1, device_id=sheet_id(dx, dy), device_id_type=MESH)

    mykind = kind(z, c)
    loads = [
        pltpu.make_async_copy(ks_ref, ksb, local_sem.at[0]),
        pltpu.make_async_copy(vs_ref, vsb, local_sem.at[1]),
    ]
    own = []
    for e in range(2):
        copies = []
        for s in range(2):
            at, span = e * 4 + s * 2 + 2, columns(s, mykind, e)
            copies += [
                pltpu.make_async_copy(k_ref.at[:, :, span], kbuf.at[e, s, 0], local_sem.at[at]),
                pltpu.make_async_copy(v_ref.at[:, :, span], vbuf.at[e, s, 0], local_sem.at[at + 1]),
            ]
        own.append(copies)
        loads = loads + copies
    for load in loads:
        load.start()

    for copy in small:
        copy.wait()
    flat = flat_ref[...].astype(jnp.float32)
    for t in range(TYPES):
        for i in range(LOCAL):
            h = 16 * (i % 4 // 2) + 4 * t + 2 * (i // 4) + i % 2
            turn2[i, 0:1, :] = flat[:, h * HEAD_DIM : (h + 1) * HEAD_DIM]
        q_ref[t] = turn2[:, 0, :].astype(jnp.bfloat16)
    own_len[...] = jnp.full((1, 128), len_ref[0], jnp.int32).astype(jnp.float32)
    offset = lax.broadcasted_iota(jnp.int32, (1, 128), 1)
    for b in range(2):
        pbuf[0, b : b + 1, :] = (table_ref[b] * 128 + offset).astype(jnp.float32)

    pl.semaphore_wait(barrier, len(line) + len(sheet))

    def remote(src, dst, send, recv, device):
        return pltpu.make_async_remote_copy(
            src_ref=src, dst_ref=dst, send_sem=send, recv_sem=recv, device_id=device, device_id_type=MESH
        )

    def line_slot(dz, dc):
        return lax.rem(z + nz - dz, nz) * 2 + lax.rem(c + dc, 2)

    def line_gather(dz, dc, slot):
        i, to = dz * 2 + dc, kind(lax.rem(z + dz, nz), lax.rem(c + dc, 2))
        device = line_id(dz, dc)
        return [
            remote(q_ref.at[to], zq.at[slot], zq_send.at[i], zq_recv.at[i], device),
            remote(own_len, zl.at[slot], zl_send.at[i], zl_recv.at[i], device),
        ]

    for dz, dc in line:
        for copy in line_gather(dz, dc, mine):
            copy.start()
    partner = {"c": other}
    places = [remote(pbuf.at[0], pbuf.at[1], kv_send.at[24], kv_recv.at[24], partner)]
    for s in range(2):
        for dc in range(2):
            i, device = 2 * s + dc, {"z": pairs[s], "c": lax.rem(c + dc, 2)}
            places.append(remote(pbuf.at[0], pbuf.at[2 + i], kv_send.at[25 + i], kv_recv.at[25 + i], device))
    swaps = []
    for e in range(2):
        copies = []
        for ref, buf, at in ((k_ref, kbuf, e * 12), (v_ref, vbuf, e * 12 + 6)):
            for s in range(2):
                for dc in range(2):
                    i, core = at + 2 + 2 * s + dc, lax.rem(c + dc, 2)
                    source = ref.at[:, :, columns(s, kind(pairs[s], core), e)]
                    device = {"z": pairs[s], "c": core}
                    copies.append(remote(source, buf.at[e, s, 2 + dc], kv_send.at[i], kv_recv.at[i], device))
            for s in range(2):
                source = ref.at[:, :, columns(s, kind(z, other), e)]
                copies.append(remote(source, buf.at[e, s, 1], kv_send.at[at + s], kv_recv.at[at + s], partner))
        swaps.append(copies)
    for copy in places + swaps[0] + swaps[1]:
        copy.start()
    zq[pl.ds(mine, 1)] = q_ref[pl.ds(mykind, 1)]
    zl[pl.ds(mine, 1)] = own_len[...][None]

    loads[0].wait()
    loads[1].wait()
    query = q_ref[...].astype(jnp.float32).reshape(HEADS, HEAD_DIM)
    place = lax.broadcasted_iota(jnp.int32, (HEADS, HEAD_DIM), 0)
    head_kv = place % 4 // 2 * 8 + place // LOCAL * 2 + place % LOCAL // 4
    own_scores = jnp.zeros((HEADS, 128), jnp.float32)
    for kv in range(KV_HEADS):
        picked = jnp.where(head_kv == kv, query, 0.0).astype(jnp.bfloat16)
        own_scores += lax.dot_general(
            picked, ksb[0, :, kv * HEAD_DIM : (kv + 1) * HEAD_DIM], NT, preferred_element_type=jnp.float32
        )
    own_scores = own_scores * SCALE2
    own_max = jnp.max(own_scores, axis=1, keepdims=True)
    own_weights = jnp.exp2(own_scores - own_max).astype(jnp.bfloat16)
    own_sum = jnp.sum(own_weights.astype(jnp.float32), axis=1, keepdims=True)
    own_out = jnp.zeros((HEADS, HEAD_DIM), jnp.float32)
    for kv in range(KV_HEADS):
        part = lax.dot_general(
            own_weights, vsb[0, :, kv * HEAD_DIM : (kv + 1) * HEAD_DIM], NN, preferred_element_type=jnp.float32
        )
        own_out += jnp.where(head_kv == kv, part, 0.0)
    so[...] = own_out
    sm[...] = jnp.broadcast_to(own_max, (HEADS, 128))
    sl[...] = jnp.broadcast_to(own_sum, (HEADS, 128))

    for dz, dc in line:
        for copy in line_gather(dz, dc, line_slot(dz, dc)):
            copy.wait_recv()
    turn[...] = zq[...].astype(jnp.float32)
    for h in range(LOCAL):
        qg[pl.ds(plane, 1), h] = turn[:, h, :].astype(jnp.bfloat16)[None]
    length = zl[:, 0, :]
    high = jnp.floor(length * (1.0 / 256.0))
    lane = lax.broadcasted_iota(jnp.int32, (rows, 128), 1)
    qg[pl.ds(plane, 1), LOCAL] = jnp.where(lane < 64, high, length - high * 256.0).astype(jnp.bfloat16)[None]

    def sheet_pass(colour, bx, by, dx, dy):
        tiles = pl.ds(0, FIRST) if colour == 0 else pl.ds(FIRST, LOCAL + 1 - FIRST)
        block = lax.rem(x + bx, nx) * ny + lax.rem(y + by, ny)
        seen = lax.rem(bx + nx - dx, nx) * ny + lax.rem(by + ny - dy, ny)
        sent = (bx + dx) * ny + dy if colour == 0 else dx * ny + by + dy
        return remote(
            qg.at[block, tiles], qg.at[block, tiles],
            xy_send.at[colour, sent], xy_recv.at[colour, seen], sheet_id(dx, dy),
        )

    def sheet_arrival(colour, bx, by):
        tiles = pl.ds(0, FIRST) if colour == 0 else pl.ds(FIRST, LOCAL + 1 - FIRST)
        block = qg.at[lax.rem(x + bx, nx) * ny + lax.rem(y + by, ny), tiles]
        i = bx * ny + by
        return remote(block, block, xy_send.at[colour, i], xy_recv.at[colour, i], sheet_id(0, 0))

    along_x = [1 + (i // 2 if i % 2 == 0 else nx - 2 - i // 2) for i in range(nx - 1)]
    along_y = [1 + (i // 2 if i % 2 == 0 else ny - 2 - i // 2) for i in range(ny - 1)]
    passes = [(0, 0, 0, dx, 0) for dx in along_x] + [(1, 0, 0, 0, dy) for dy in along_y]
    passes += [(0, 0, 0, 0, dy) for dy in along_y] + [(1, 0, 0, dx, 0) for dx in along_x]
    for step in passes:
        sheet_pass(*step).start()
    seen_first = [(0, bx, 0) for bx in along_x] + [(1, 0, by) for by in along_y]
    for colour, bx, by in sorted(seen_first, key=lambda b: (along_x + along_y).index(b[1] + b[2])):
        sheet_arrival(colour, bx, by).wait_recv()
        onward = [(0, bx, 0, 0, dy) for dy in along_y] if colour == 0 else [(1, 0, by, dx, 0) for dx in along_x]
        for step in onward:
            sheet_pass(*step).start()
        passes += onward

    for copy in places:
        copy.wait_recv()
    tokens = 8 * 128
    positions = [
        jnp.concatenate([pbuf[p, b : b + 1, :] for p in (0, 1, 2 + 2 * s, 3 + 2 * s) for b in range(2)], axis=1)
        for s in range(2)
    ]
    ones = jnp.ones((tokens, HEAD_DIM), jnp.bfloat16)
    group = ny * 2 * rows
    pile = min(rows, 8)

    def packed(tile):
        tile = tile.reshape(-1, pile, 128)
        line = sum(pltpu.roll(tile[i], 64 * i, 1, stride=8, stride_axis=0) for i in range(rows // pile))
        return jnp.sum(line, axis=0, keepdims=True)

    def sheet_return(e, i, device, here, there):
        return [
            remote(osend.at[e, here], orecv.at[e, there], ro_send.at[e, i], ro_recv.at[e, i], device),
            remote(msend.at[e, here], mrecv.at[e, there], rm_send.at[e, i], rm_recv.at[e, i], device),
        ]

    def chunk(e, k):
        column = lax.rem(x + k, nx)
        base = column * ny
        if e == 0:
            for dy in range(1, ny):
                sheet_arrival(0, k, dy).wait_recv()

            def arrive():
                for dy in range(ny):
                    sheet_arrival(1, k, dy).wait_recv()

            pl.when(k > 0)(arrive)
        tile = qg[pl.ds(base, ny), LOCAL].astype(jnp.float32)
        wide = tile[:, :, 0:1] * 256.0 + tile[:, :, 64:65]
        limit = jnp.broadcast_to(wide[:, None], (ny, 2, rows, 1)).reshape(group, 1)
        lanes = lax.broadcasted_iota(jnp.int32, (ny, rows, 128), 2)
        stats = jnp.zeros((ny, rows, 128), jnp.float32)
        for s in range(2):
            g = 2 * e + s
            queries = qg[pl.ds(base, ny), 2 * g : 2 * g + 2].reshape(group, HEAD_DIM)
            keys = kbuf[e, s].reshape(tokens, HEAD_DIM)
            values = vbuf[e, s].reshape(tokens, HEAD_DIM)
            scores = lax.dot_general(queries, keys, NT, preferred_element_type=jnp.float32) * SCALE2
            scores = jnp.where(positions[s] < limit, scores, MASKED)
            top = jnp.maximum(jnp.max(scores, axis=1, keepdims=True), FLOOR)
            weights = jnp.exp2(scores - top).astype(jnp.bfloat16)
            both = lax.dot_general(
                weights, jnp.concatenate([values, ones], axis=1), NN, preferred_element_type=jnp.float32
            )
            osend[e, pl.ds(base, ny), 2 * s : 2 * s + 2] = (
                both[:, :HEAD_DIM].astype(jnp.bfloat16).reshape(ny, 2, rows, HEAD_DIM)
            )
            tops = jnp.broadcast_to(top, (group, 128)).reshape(ny, 2, rows, 128)
            sums = both[:, HEAD_DIM:].reshape(ny, 2, rows, 128)
            for j in range(2):
                stats = jnp.where(lanes == 2 * s + j, tops[:, j], stats)
                stats = jnp.where(lanes == 4 + 2 * s + j, sums[:, j], stats)
        for i in range(ny):
            msend[e, pl.ds(base + i, 1)] = packed(stats[i])[None]
        for dy in range(ny):
            row = lax.rem(y + dy, ny)
            there = column * ny + row

            def leave(dy=dy, row=row, there=there):
                for copy in sheet_return(e, k * ny + dy, {"x": column, "y": row}, there, plane):
                    copy.start()

            if dy == 0:
                pl.when(k > 0)(leave)
            else:
                leave()

    for e in range(2):
        for copy in own[e]:
            copy.wait()
        for copy in swaps[e]:
            copy.wait_recv()
        lax.fori_loop(0, nx, lambda k, carry, e=e: (chunk(e, lax.rem(k + e, nx)), carry)[1], 0)
        orecv[e, pl.ds(plane, 1)] = osend[e, pl.ds(plane, 1)]
        mrecv[e, pl.ds(plane, 1)] = msend[e, pl.ds(plane, 1)]

    def line_return(e, dz, dc, here, there):
        i = dz * 2 + dc
        device = line_id(dz, dc)
        return [
            remote(osend2.at[e, here], orecv2.at[e, there], fo_send.at[e, i], fo_recv.at[e, i], device),
            remote(msend2.at[e], mrecv2.at[e, there], fm_send.at[e, i], fm_recv.at[e, i], device),
        ]

    count = nx * ny
    at_row = lax.broadcasted_iota(jnp.int32, (rows, 128), 0) * 8
    zero = jnp.zeros((rows, HEAD_DIM), jnp.float32)
    for e in range(2):
        for dx, dy in sheet:
            slot = lax.rem(x + nx - dx, nx) * ny + lax.rem(y + ny - dy, ny)
            for copy in sheet_return(e, dx * ny + dy, sheet_id(dx, dy), slot, slot):
                copy.wait_recv()
        best = jnp.max(mrecv[e], axis=0)

        def merge(s, carry, e=e, best=best):
            total, out = carry
            part = mrecv[e, pl.ds(s, 1)][0]
            factor = jnp.exp2(part - best)
            total = total + pltpu.roll(factor, 4, 1) * part
            spread = jnp.broadcast_to(factor, (rows, 128))
            block = orecv[e, pl.ds(s, 1)][0].astype(jnp.float32)
            out = tuple(
                out[h] + jnp.sum(jnp.where(lane == at_row + h, spread, 0.0), axis=1, keepdims=True) * block[h]
                for h in range(4)
            )
            return total, out

        total, out = lax.fori_loop(0, count, merge, (jnp.zeros_like(best), (zero,) * 4), unroll=4)
        msend2[e] = jnp.where(lane[:1] % 8 < 4, best, total)
        for h in range(4):
            turn2[4 * e + h] = out[h]
        for r in range(rows):
            osend2[e, r] = turn2[4 * e : 4 * e + 4, r, :]
        for dz, dc in line:
            target = lax.rem(z + dz, nz) * 2 + lax.rem(c + dc, 2)
            for copy in line_return(e, dz, dc, target, mine):
                copy.start()
        orecv2[e, pl.ds(mine, 1)] = osend2[e, pl.ds(mine, 1)]
        mrecv2[e, pl.ds(mine, 1)] = msend2[e][None]

    lane_of = lax.broadcasted_iota(jnp.int32, (4, 128), 1)
    line_log = jnp.zeros((1, 128), jnp.float32)
    head_row = lax.broadcasted_iota(jnp.int32, (4, 128), 0)
    pick = mine * 8 + lax.broadcasted_iota(jnp.int32, (4, 128), 0)
    for e in range(2):
        for dz, dc in line:
            slot = line_slot(dz, dc)
            for copy in line_return(e, dz, dc, slot, slot):
                copy.wait_recv()
        for t in range(TYPES):
            heads = slice(t * LOCAL + 4 * e, t * LOCAL + 4 * e + 4)
            slots = [zz * 2 + t % 2 for zz in range(nz) if zz % 2 == t // 2]
            tops, sums = [sm[heads, 0:1]], [sl[heads, 0:1]]
            for slot in slots:
                row = jnp.broadcast_to(mrecv2[e, slot], (4, 128))
                tops.append(jnp.sum(jnp.where(lane_of == pick, row, 0.0), axis=1, keepdims=True))
                sums.append(jnp.sum(jnp.where(lane_of == pick + 4, row, 0.0), axis=1, keepdims=True))
            top = functools.reduce(jnp.maximum, tops)
            factors = [jnp.exp2(m - top) for m in tops]
            normalizer = sum(f * l for f, l in zip(factors, sums))
            numerator = factors[0] * so[heads, :]
            for f, slot in zip(factors[1:], slots):
                numerator += f * orecv2[e, slot]
            numerator = numerator / normalizer
            logs = jnp.broadcast_to(top * LN2 + jnp.log(normalizer), (4, 128))
            wanted = 16 * (head_row // 2) + 4 * t + 2 * e + head_row % 2
            line_log += jnp.sum(jnp.where(lane_of == wanted, logs, 0.0), axis=0, keepdims=True)
            for s in range(2):
                first = 16 * s + 4 * t + 2 * e
                natural[first : first + 2, :] = numerator[2 * s : 2 * s + 2]
    for h in range(HEADS):
        out_ref[:, h * HEAD_DIM : (h + 1) * HEAD_DIM] = natural[h : h + 1, :].astype(jnp.bfloat16)
    log_ref[...] = line_log[:, :HEADS]

    for copy in places + swaps[0] + swaps[1]:
        copy.wait_send()
    for step in passes:
        sheet_pass(*step).wait_send()
    for dz, dc in line:
        target = lax.rem(z + dz, nz) * 2 + lax.rem(c + dc, 2)
        for copy in line_gather(dz, dc, mine):
            copy.wait_send()
        for e in range(2):
            for copy in line_return(e, dz, dc, target, mine):
                copy.wait_send()
    for dx, dy in sheet:
        i, device = dx * ny + dy, sheet_id(dx, dy)
        there = lax.rem(x + dx, nx) * ny + lax.rem(y + dy, ny)
        for e in range(2):
            for copy in sheet_return(e, i, device, there, plane):
                copy.wait_send()


def body(nx, ny, nz, queries, prefix_len, prefix_keys, prefix_values, block_table, suffix_keys, suffix_values):
    rows, count = nz * 2, nx * ny
    vmem, hbm = pl.BlockSpec(memory_space=pltpu.VMEM), pl.BlockSpec(memory_space=pltpu.HBM)
    bf16, f32 = jnp.bfloat16, jnp.float32
    dma = pltpu.SemaphoreType.DMA
    out, logs = pl.pallas_call(
        kernel,
        name="decode",
        out_shape=[
            jax.ShapeDtypeStruct((1, HEADS * HEAD_DIM), bf16),
            jax.ShapeDtypeStruct((1, HEADS), f32),
        ],
        in_specs=[hbm, hbm, hbm, hbm, hbm, hbm, hbm],
        out_specs=[vmem, vmem],
        scratch_shapes=[
            pltpu.VMEM((1, HEADS * HEAD_DIM), bf16),
            pltpu.SMEM((1,), jnp.int32),
            pltpu.SMEM((2,), jnp.int32),
            pltpu.VMEM((TYPES, LOCAL, HEAD_DIM), bf16),
            pltpu.VMEM((1, 128), f32),
            pltpu.VMEM((rows, LOCAL, HEAD_DIM), bf16),
            pltpu.VMEM((rows, 1, 128), f32),
            pltpu.VMEM((rows, LOCAL, HEAD_DIM), f32),
            pltpu.VMEM((LOCAL, rows, HEAD_DIM), f32),
            pltpu.VMEM((count, LOCAL + 1, rows, HEAD_DIM), bf16),
            pltpu.VMEM((2, 2, 4, 2, 128, HEAD_DIM), bf16),
            pltpu.VMEM((2, 2, 4, 2, 128, HEAD_DIM), bf16),
            pltpu.VMEM((6, 8, 128), f32),
            pltpu.VMEM((1, 128, KV_HEADS * HEAD_DIM), bf16),
            pltpu.VMEM((1, 128, KV_HEADS * HEAD_DIM), bf16),
            pltpu.VMEM((2, count, 4, rows, HEAD_DIM), bf16),
            pltpu.VMEM((2, count, 1, 128), f32),
            pltpu.VMEM((2, count, 4, rows, HEAD_DIM), bf16),
            pltpu.VMEM((2, count, 1, 128), f32),
            pltpu.VMEM((2, rows, 4, HEAD_DIM), f32),
            pltpu.VMEM((2, 1, 128), f32),
            pltpu.VMEM((2, rows, 4, HEAD_DIM), f32),
            pltpu.VMEM((2, rows, 1, 128), f32),
            pltpu.VMEM((HEADS, HEAD_DIM), f32),
            pltpu.VMEM((HEADS, 128), f32),
            pltpu.VMEM((HEADS, 128), f32),
            pltpu.VMEM((HEADS, HEAD_DIM), f32),
            dma((3,)), dma((10,)), dma((29,)), dma((29,)),
            dma((rows,)), dma((rows,)), dma((rows,)), dma((rows,)),
            dma((2, count)), dma((2, count)),
            dma((2, count)), dma((2, count)), dma((2, count)), dma((2, count)),
            dma((2, rows)), dma((2, rows)), dma((2, rows)), dma((2, rows)),
        ],
        compiler_params=pltpu.CompilerParams(
            collective_id=0, has_side_effects=True, vmem_limit_bytes=63 * 1024 * 1024
        ),
    )(queries, prefix_len, block_table, prefix_keys, prefix_values, suffix_keys, suffix_values)
    return out, logs


def sizes(mesh):
    nx = mesh.shape["grp"]
    nz = 8 if mesh.shape["hold"] == 64 else 2
    return nx, mesh.shape["hold"] // (2 * nz), nz


def solution(mesh):
    nx, ny, nz = sizes(mesh)
    split = Mesh(mesh.devices.reshape(nx, ny, nz, 2), AXES)
    rows = P(AXES, None)
    return jax.shard_map(
        functools.partial(body, nx, ny, nz),
        mesh=split,
        in_specs=(rows, P(AXES), P(AXES, None, None), P(AXES, None, None), P(AXES), P(AXES, None, None), P(AXES, None, None)),
        out_specs=(rows, rows),
        check_vma=False,
    )
```

```python
import functools
import math

import jax
import jax.numpy as jnp
from jax import lax
from jax.experimental import pallas as pl
from jax.experimental.pallas import tpu as pltpu
from jax.sharding import Mesh
from jax.sharding import PartitionSpec as P

HEADS = 32
KV_HEADS = 16
HEAD_DIM = 128
TYPES = 4
LOCAL = HEADS // TYPES
FIRST = LOCAL // 2
AXES = ("x", "y", "z", "c")
MESH = pl.DeviceIdType.MESH

SCALE2 = math.log2(math.e) / 168.0**0.5
LN2 = math.log(2.0)
MASKED = -1e30
FLOOR = -1e29

NT = (((1,), (1,)), ((), ()))
NN = (((1,), (0,)), ((), ()))


def kernel(
    flat_hbm, len_hbm, table_hbm, k_ref, v_ref, ks_ref, vs_ref,
    out_ref, log_ref,
    flat_ref, len_ref, table_ref, q_ref, own_len, zq, zl, turn, turn2, qg, kbuf, vbuf, pbuf, ksb, vsb,
    osend, msend, orecv, mrecv, osend2, msend2, orecv2, mrecv2, so, sm, sl, natural,
    small_sem, local_sem, kv_send, kv_recv, zq_send, zq_recv, zl_send, zl_recv,
    xy_send, xy_recv, ro_send, ro_recv, rm_send, rm_recv,
    fo_send, fo_recv, fm_send, fm_recv,
):
    nx, ny, nz = (lax.axis_size(a) for a in AXES[:3])
    x, y, z, c = (lax.axis_index(a) for a in AXES)
    rows = nz * 2
    mine, plane = z * 2 + c, x * ny + y
    other = 1 - c
    odd = lax.rem(z, 2)
    pairs = [z + 1 - 2 * odd, lax.rem(z + nz - 1 + 2 * odd, nz)]

    def kind(zz, cc):
        return lax.rem(zz, 2) * 2 + cc

    def columns(s, t, e):
        return pl.ds(pl.multiple_of((s * 8 + t * 2 + e) * HEAD_DIM, HEAD_DIM), HEAD_DIM)

    small = [
        pltpu.make_async_copy(src, dst, small_sem.at[i])
        for i, (src, dst) in enumerate([(flat_hbm, flat_ref), (len_hbm, len_ref), (table_hbm, table_ref)])
    ]
    for copy in small:
        copy.start()
    line = [(dz, dc) for dz in range(nz) for dc in range(2) if (dz, dc) != (0, 0)]
    line.sort(key=lambda d: -min(d[0], nz - d[0]))
    sheet = [(dx, dy) for dx in range(nx) for dy in range(ny) if (dx, dy) != (0, 0)]
    sheet.sort(key=lambda d: -min(d[0], nx - d[0]) - min(d[1], ny - d[1]))

    def line_id(dz, dc):
        return {"z": lax.rem(z + dz, nz), "c": lax.rem(c + dc, 2)}

    def sheet_id(dx, dy):
        return {"x": lax.rem(x + dx, nx), "y": lax.rem(y + dy, ny)}

    barrier = pltpu.get_barrier_semaphore()
    for dz, dc in line:
        pl.semaphore_signal(barrier, inc=1, device_id=line_id(dz, dc), device_id_type=MESH)
    for dx, dy in sheet:
        pl.semaphore_signal(barrier, inc=1, device_id=sheet_id(dx, dy), device_id_type=MESH)

    mykind = kind(z, c)
    loads = [
        pltpu.make_async_copy(ks_ref, ksb, local_sem.at[0]),
        pltpu.make_async_copy(vs_ref, vsb, local_sem.at[1]),
    ]
    own = []
    for e in range(2):
        copies = []
        for s in range(2):
            at, span = e * 4 + s * 2 + 2, columns(s, mykind, e)
            copies += [
                pltpu.make_async_copy(k_ref.at[:, :, span], kbuf.at[e, s, 0], local_sem.at[at]),
                pltpu.make_async_copy(v_ref.at[:, :, span], vbuf.at[e, s, 0], local_sem.at[at + 1]),
            ]
        own.append(copies)
        loads = loads + copies
    for load in loads:
        load.start()

    for copy in small:
        copy.wait()
    flat = flat_ref[...].astype(jnp.float32)
    for t in range(TYPES):
        for i in range(LOCAL):
            h = 16 * (i % 4 // 2) + 4 * t + 2 * (i // 4) + i % 2
            turn2[i, 0:1, :] = flat[:, h * HEAD_DIM : (h + 1) * HEAD_DIM]
        q_ref[t] = turn2[:, 0, :].astype(jnp.bfloat16)
    own_len[...] = jnp.full((1, 128), len_ref[0], jnp.int32).astype(jnp.float32)
    offset = lax.broadcasted_iota(jnp.int32, (1, 128), 1)
    for b in range(2):
        pbuf[0, b : b + 1, :] = (table_ref[b] * 128 + offset).astype(jnp.float32)

    pl.semaphore_wait(barrier, len(line) + len(sheet))

    def remote(src, dst, send, recv, device):
        return pltpu.make_async_remote_copy(
            src_ref=src, dst_ref=dst, send_sem=send, recv_sem=recv, device_id=device, device_id_type=MESH
        )

    def line_slot(dz, dc):
        return lax.rem(z + nz - dz, nz) * 2 + lax.rem(c + dc, 2)

    def line_gather(dz, dc, slot):
        i, to = dz * 2 + dc, kind(lax.rem(z + dz, nz), lax.rem(c + dc, 2))
        device = line_id(dz, dc)
        return [
            remote(q_ref.at[to], zq.at[slot], zq_send.at[i], zq_recv.at[i], device),
            remote(own_len, zl.at[slot], zl_send.at[i], zl_recv.at[i], device),
        ]

    for dz, dc in line:
        for copy in line_gather(dz, dc, mine):
            copy.start()
    partner = {"c": other}
    places = [remote(pbuf.at[0], pbuf.at[1], kv_send.at[24], kv_recv.at[24], partner)]
    for s in range(2):
        for dc in range(2):
            i, device = 2 * s + dc, {"z": pairs[s], "c": lax.rem(c + dc, 2)}
            places.append(remote(pbuf.at[0], pbuf.at[2 + i], kv_send.at[25 + i], kv_recv.at[25 + i], device))
    swaps = []
    for e in range(2):
        copies = []
        for ref, buf, at in ((k_ref, kbuf, e * 12), (v_ref, vbuf, e * 12 + 6)):
            for s in range(2):
                for dc in range(2):
                    i, core = at + 2 + 2 * s + dc, lax.rem(c + dc, 2)
                    source = ref.at[:, :, columns(s, kind(pairs[s], core), e)]
                    device = {"z": pairs[s], "c": core}
                    copies.append(remote(source, buf.at[e, s, 2 + dc], kv_send.at[i], kv_recv.at[i], device))
            for s in range(2):
                source = ref.at[:, :, columns(s, kind(z, other), e)]
                copies.append(remote(source, buf.at[e, s, 1], kv_send.at[at + s], kv_recv.at[at + s], partner))
        swaps.append(copies)
    for copy in places + swaps[0] + swaps[1]:
        copy.start()
    zq[pl.ds(mine, 1)] = q_ref[pl.ds(mykind, 1)]
    zl[pl.ds(mine, 1)] = own_len[...][None]

    loads[0].wait()
    loads[1].wait()
    query = q_ref[...].astype(jnp.float32).reshape(HEADS, HEAD_DIM)
    place = lax.broadcasted_iota(jnp.int32, (HEADS, HEAD_DIM), 0)
    head_kv = place % 4 // 2 * 8 + place // LOCAL * 2 + place % LOCAL // 4
    own_scores = jnp.zeros((HEADS, 128), jnp.float32)
    for kv in range(KV_HEADS):
        picked = jnp.where(head_kv == kv, query, 0.0).astype(jnp.bfloat16)
        own_scores += lax.dot_general(
            picked, ksb[0, :, kv * HEAD_DIM : (kv + 1) * HEAD_DIM], NT, preferred_element_type=jnp.float32
        )
    own_scores = own_scores * SCALE2
    own_max = jnp.max(own_scores, axis=1, keepdims=True)
    own_weights = jnp.exp2(own_scores - own_max).astype(jnp.bfloat16)
    own_sum = jnp.sum(own_weights.astype(jnp.float32), axis=1, keepdims=True)
    own_out = jnp.zeros((HEADS, HEAD_DIM), jnp.float32)
    for kv in range(KV_HEADS):
        part = lax.dot_general(
            own_weights, vsb[0, :, kv * HEAD_DIM : (kv + 1) * HEAD_DIM], NN, preferred_element_type=jnp.float32
        )
        own_out += jnp.where(head_kv == kv, part, 0.0)
    so[...] = own_out
    sm[...] = jnp.broadcast_to(own_max, (HEADS, 128))
    sl[...] = jnp.broadcast_to(own_sum, (HEADS, 128))

    for dz, dc in line:
        for copy in line_gather(dz, dc, line_slot(dz, dc)):
            copy.wait_recv()
    turn[...] = zq[...].astype(jnp.float32)
    for h in range(LOCAL):
        qg[pl.ds(plane, 1), h] = turn[:, h, :].astype(jnp.bfloat16)[None]
    length = zl[:, 0, :]
    high = jnp.floor(length * (1.0 / 256.0))
    lane = lax.broadcasted_iota(jnp.int32, (rows, 128), 1)
    qg[pl.ds(plane, 1), LOCAL] = jnp.where(lane < 64, high, length - high * 256.0).astype(jnp.bfloat16)[None]

    def sheet_pass(colour, bx, by, dx, dy):
        tiles = pl.ds(0, FIRST) if colour == 0 else pl.ds(FIRST, LOCAL + 1 - FIRST)
        block = lax.rem(x + bx, nx) * ny + lax.rem(y + by, ny)
        seen = lax.rem(bx + nx - dx, nx) * ny + lax.rem(by + ny - dy, ny)
        sent = (bx + dx) * ny + dy if colour == 0 else dx * ny + by + dy
        return remote(
            qg.at[block, tiles], qg.at[block, tiles],
            xy_send.at[colour, sent], xy_recv.at[colour, seen], sheet_id(dx, dy),
        )

    def sheet_arrival(colour, bx, by):
        tiles = pl.ds(0, FIRST) if colour == 0 else pl.ds(FIRST, LOCAL + 1 - FIRST)
        block = qg.at[lax.rem(x + bx, nx) * ny + lax.rem(y + by, ny), tiles]
        i = bx * ny + by
        return remote(block, block, xy_send.at[colour, i], xy_recv.at[colour, i], sheet_id(0, 0))

    along_x = [1 + (i // 2 if i % 2 == 0 else nx - 2 - i // 2) for i in range(nx - 1)]
    along_y = [1 + (i // 2 if i % 2 == 0 else ny - 2 - i // 2) for i in range(ny - 1)]
    passes = [(0, 0, 0, dx, 0) for dx in along_x] + [(1, 0, 0, 0, dy) for dy in along_y]
    passes += [(0, 0, 0, 0, dy) for dy in along_y] + [(1, 0, 0, dx, 0) for dx in along_x]
    for step in passes:
        sheet_pass(*step).start()
    seen_first = [(0, bx, 0) for bx in along_x] + [(1, 0, by) for by in along_y]
    for colour, bx, by in sorted(seen_first, key=lambda b: (along_x + along_y).index(b[1] + b[2])):
        sheet_arrival(colour, bx, by).wait_recv()
        onward = [(0, bx, 0, 0, dy) for dy in along_y] if colour == 0 else [(1, 0, by, dx, 0) for dx in along_x]
        for step in onward:
            sheet_pass(*step).start()
        passes += onward

    for copy in places:
        copy.wait_recv()
    tokens = 8 * 128
    positions = [
        jnp.concatenate([pbuf[p, b : b + 1, :] for p in (0, 1, 2 + 2 * s, 3 + 2 * s) for b in range(2)], axis=1)
        for s in range(2)
    ]
    ones = jnp.ones((tokens, HEAD_DIM), jnp.bfloat16)
    group = ny * 2 * rows
    pile = min(rows, 8)

    def packed(tile):
        tile = tile.reshape(-1, pile, 128)
        line = sum(pltpu.roll(tile[i], 64 * i, 1, stride=8, stride_axis=0) for i in range(rows // pile))
        return jnp.sum(line, axis=0, keepdims=True)

    def sheet_return(e, i, device, here, there):
        return [
            remote(osend.at[e, here], orecv.at[e, there], ro_send.at[e, i], ro_recv.at[e, i], device),
            remote(msend.at[e, here], mrecv.at[e, there], rm_send.at[e, i], rm_recv.at[e, i], device),
        ]

    def chunk(e, k):
        column = lax.rem(x + k, nx)
        base = column * ny
        if e == 0:
            for dy in range(1, ny):
                sheet_arrival(0, k, dy).wait_recv()

            def arrive():
                for dy in range(ny):
                    sheet_arrival(1, k, dy).wait_recv()

            pl.when(k > 0)(arrive)
        tile = qg[pl.ds(base, ny), LOCAL].astype(jnp.float32)
        wide = tile[:, :, 0:1] * 256.0 + tile[:, :, 64:65]
        limit = jnp.broadcast_to(wide[:, None], (ny, 2, rows, 1)).reshape(group, 1)
        lanes = lax.broadcasted_iota(jnp.int32, (ny, rows, 128), 2)
        stats = jnp.zeros((ny, rows, 128), jnp.float32)
        for s in range(2):
            g = 2 * e + s
            queries = qg[pl.ds(base, ny), 2 * g : 2 * g + 2].reshape(group, HEAD_DIM)
            keys = kbuf[e, s].reshape(tokens, HEAD_DIM)
            values = vbuf[e, s].reshape(tokens, HEAD_DIM)
            scores = lax.dot_general(queries, keys, NT, preferred_element_type=jnp.float32) * SCALE2
            scores = jnp.where(positions[s] < limit, scores, MASKED)
            top = jnp.maximum(jnp.max(scores, axis=1, keepdims=True), FLOOR)
            weights = jnp.exp2(scores - top).astype(jnp.bfloat16)
            both = lax.dot_general(
                weights, jnp.concatenate([values, ones], axis=1), NN, preferred_element_type=jnp.float32
            )
            osend[e, pl.ds(base, ny), 2 * s : 2 * s + 2] = (
                both[:, :HEAD_DIM].astype(jnp.bfloat16).reshape(ny, 2, rows, HEAD_DIM)
            )
            tops = jnp.broadcast_to(top, (group, 128)).reshape(ny, 2, rows, 128)
            sums = both[:, HEAD_DIM:].reshape(ny, 2, rows, 128)
            for j in range(2):
                stats = jnp.where(lanes == 2 * s + j, tops[:, j], stats)
                stats = jnp.where(lanes == 4 + 2 * s + j, sums[:, j], stats)
        for i in range(ny):
            msend[e, pl.ds(base + i, 1)] = packed(stats[i])[None]
        for dy in range(ny):
            row = lax.rem(y + dy, ny)
            there = column * ny + row

            def leave(dy=dy, row=row, there=there):
                for copy in sheet_return(e, k * ny + dy, {"x": column, "y": row}, there, plane):
                    copy.start()

            if dy == 0:
                pl.when(k > 0)(leave)
            else:
                leave()

    for e in range(2):
        for copy in own[e]:
            copy.wait()
        for copy in swaps[e]:
            copy.wait_recv()
        lax.fori_loop(0, nx, lambda k, carry, e=e: (chunk(e, lax.rem(k + e, nx)), carry)[1], 0)
        orecv[e, pl.ds(plane, 1)] = osend[e, pl.ds(plane, 1)]
        mrecv[e, pl.ds(plane, 1)] = msend[e, pl.ds(plane, 1)]

    def line_return(e, dz, dc, here, there):
        i = dz * 2 + dc
        device = line_id(dz, dc)
        return [
            remote(osend2.at[e, here], orecv2.at[e, there], fo_send.at[e, i], fo_recv.at[e, i], device),
            remote(msend2.at[e], mrecv2.at[e, there], fm_send.at[e, i], fm_recv.at[e, i], device),
        ]

    count = nx * ny
    at_row = lax.broadcasted_iota(jnp.int32, (rows, 128), 0) * 8
    zero = jnp.zeros((rows, HEAD_DIM), jnp.float32)
    for e in range(2):
        for dx, dy in sheet:
            slot = lax.rem(x + nx - dx, nx) * ny + lax.rem(y + ny - dy, ny)
            for copy in sheet_return(e, dx * ny + dy, sheet_id(dx, dy), slot, slot):
                copy.wait_recv()
        best = jnp.max(mrecv[e], axis=0)

        def merge(s, carry, e=e, best=best):
            total, out = carry
            part = mrecv[e, pl.ds(s, 1)][0]
            factor = jnp.exp2(part - best)
            total = total + pltpu.roll(factor, 4, 1) * part
            spread = jnp.broadcast_to(factor, (rows, 128))
            block = orecv[e, pl.ds(s, 1)][0].astype(jnp.float32)
            out = tuple(
                out[h] + jnp.sum(jnp.where(lane == at_row + h, spread, 0.0), axis=1, keepdims=True) * block[h]
                for h in range(4)
            )
            return total, out

        total, out = lax.fori_loop(0, count, merge, (jnp.zeros_like(best), (zero,) * 4), unroll=4)
        msend2[e] = jnp.where(lane[:1] % 8 < 4, best, total)
        for h in range(4):
            turn2[4 * e + h] = out[h]
        for r in range(rows):
            osend2[e, r] = turn2[4 * e : 4 * e + 4, r, :]
        for dz, dc in line:
            target = lax.rem(z + dz, nz) * 2 + lax.rem(c + dc, 2)
            for copy in line_return(e, dz, dc, target, mine):
                copy.start()
        orecv2[e, pl.ds(mine, 1)] = osend2[e, pl.ds(mine, 1)]
        mrecv2[e, pl.ds(mine, 1)] = msend2[e][None]

    for copy in places + swaps[0] + swaps[1]:
        copy.wait_send()
    for step in passes:
        sheet_pass(*step).wait_send()
    for dz, dc in line:
        target = lax.rem(z + dz, nz) * 2 + lax.rem(c + dc, 2)
        for copy in line_gather(dz, dc, mine):
            copy.wait_send()
        for e in range(2):
            for copy in line_return(e, dz, dc, target, mine):
                copy.wait_send()
    for dx, dy in sheet:
        i, device = dx * ny + dy, sheet_id(dx, dy)
        there = lax.rem(x + dx, nx) * ny + lax.rem(y + dy, ny)
        for e in range(2):
            for copy in sheet_return(e, i, device, there, plane):
                copy.wait_send()

    lane_of = lax.broadcasted_iota(jnp.int32, (4, 128), 1)
    line_log = jnp.zeros((1, 128), jnp.float32)
    head_row = lax.broadcasted_iota(jnp.int32, (4, 128), 0)
    pick = mine * 8 + lax.broadcasted_iota(jnp.int32, (4, 128), 0)
    for e in range(2):
        for dz, dc in line:
            slot = line_slot(dz, dc)
            for copy in line_return(e, dz, dc, slot, slot):
                copy.wait_recv()
        for t in range(TYPES):
            heads = slice(t * LOCAL + 4 * e, t * LOCAL + 4 * e + 4)
            slots = [zz * 2 + t % 2 for zz in range(nz) if zz % 2 == t // 2]
            tops, sums = [sm[heads, 0:1]], [sl[heads, 0:1]]
            for slot in slots:
                row = jnp.broadcast_to(mrecv2[e, slot], (4, 128))
                tops.append(jnp.sum(jnp.where(lane_of == pick, row, 0.0), axis=1, keepdims=True))
                sums.append(jnp.sum(jnp.where(lane_of == pick + 4, row, 0.0), axis=1, keepdims=True))
            top = functools.reduce(jnp.maximum, tops)
            factors = [jnp.exp2(m - top) for m in tops]
            normalizer = sum(f * l for f, l in zip(factors, sums))
            numerator = factors[0] * so[heads, :]
            for f, slot in zip(factors[1:], slots):
                numerator += f * orecv2[e, slot]
            numerator = numerator / normalizer
            logs = jnp.broadcast_to(top * LN2 + jnp.log(normalizer), (4, 128))
            wanted = 16 * (head_row // 2) + 4 * t + 2 * e + head_row % 2
            line_log += jnp.sum(jnp.where(lane_of == wanted, logs, 0.0), axis=0, keepdims=True)
            for s in range(2):
                first = 16 * s + 4 * t + 2 * e
                natural[first : first + 2, :] = numerator[2 * s : 2 * s + 2]
    for h in range(HEADS):
        out_ref[:, h * HEAD_DIM : (h + 1) * HEAD_DIM] = natural[h : h + 1, :].astype(jnp.bfloat16)
    log_ref[...] = line_log[:, :HEADS]


def settle(out_ref, log_ref, out_final, log_final):
    out_final[...] = out_ref[...]
    log_final[...] = log_ref[...]


def body(nx, ny, nz, queries, prefix_len, prefix_keys, prefix_values, block_table, suffix_keys, suffix_values):
    rows, count = nz * 2, nx * ny
    vmem, hbm = pl.BlockSpec(memory_space=pltpu.VMEM), pl.BlockSpec(memory_space=pltpu.HBM)
    bf16, f32 = jnp.bfloat16, jnp.float32
    dma = pltpu.SemaphoreType.DMA
    out, logs = pl.pallas_call(
        kernel,
        name="decode",
        out_shape=[
            pltpu.VMEM((1, HEADS * HEAD_DIM), bf16),
            pltpu.VMEM((1, HEADS), f32),
        ],
        in_specs=[hbm, hbm, hbm, hbm, hbm, hbm, hbm],
        out_specs=[vmem, vmem],
        scratch_shapes=[
            pltpu.VMEM((1, HEADS * HEAD_DIM), bf16),
            pltpu.SMEM((1,), jnp.int32),
            pltpu.SMEM((2,), jnp.int32),
            pltpu.VMEM((TYPES, LOCAL, HEAD_DIM), bf16),
            pltpu.VMEM((1, 128), f32),
            pltpu.VMEM((rows, LOCAL, HEAD_DIM), bf16),
            pltpu.VMEM((rows, 1, 128), f32),
            pltpu.VMEM((rows, LOCAL, HEAD_DIM), f32),
            pltpu.VMEM((LOCAL, rows, HEAD_DIM), f32),
            pltpu.VMEM((count, LOCAL + 1, rows, HEAD_DIM), bf16),
            pltpu.VMEM((2, 2, 4, 2, 128, HEAD_DIM), bf16),
            pltpu.VMEM((2, 2, 4, 2, 128, HEAD_DIM), bf16),
            pltpu.VMEM((6, 8, 128), f32),
            pltpu.VMEM((1, 128, KV_HEADS * HEAD_DIM), bf16),
            pltpu.VMEM((1, 128, KV_HEADS * HEAD_DIM), bf16),
            pltpu.VMEM((2, count, 4, rows, HEAD_DIM), bf16),
            pltpu.VMEM((2, count, 1, 128), f32),
            pltpu.VMEM((2, count, 4, rows, HEAD_DIM), bf16),
            pltpu.VMEM((2, count, 1, 128), f32),
            pltpu.VMEM((2, rows, 4, HEAD_DIM), f32),
            pltpu.VMEM((2, 1, 128), f32),
            pltpu.VMEM((2, rows, 4, HEAD_DIM), f32),
            pltpu.VMEM((2, rows, 1, 128), f32),
            pltpu.VMEM((HEADS, HEAD_DIM), f32),
            pltpu.VMEM((HEADS, 128), f32),
            pltpu.VMEM((HEADS, 128), f32),
            pltpu.VMEM((HEADS, HEAD_DIM), f32),
            dma((3,)), dma((10,)), dma((29,)), dma((29,)),
            dma((rows,)), dma((rows,)), dma((rows,)), dma((rows,)),
            dma((2, count)), dma((2, count)),
            dma((2, count)), dma((2, count)), dma((2, count)), dma((2, count)),
            dma((2, rows)), dma((2, rows)), dma((2, rows)), dma((2, rows)),
        ],
        compiler_params=pltpu.CompilerParams(
            collective_id=0, has_side_effects=True, vmem_limit_bytes=63 * 1024 * 1024
        ),
    )(queries, prefix_len, block_table, prefix_keys, prefix_values, suffix_keys, suffix_values)
    return tuple(pl.pallas_call(
        settle,
        name="settle",
        out_shape=[jax.ShapeDtypeStruct(out.shape, bf16), jax.ShapeDtypeStruct(logs.shape, f32)],
        in_specs=[vmem, vmem],
        out_specs=[vmem, vmem],
    )(*(pltpu.with_memory_space_constraint(a, pltpu.VMEM) for a in (out, logs))))


def sizes(mesh):
    nx = mesh.shape["grp"]
    nz = 8 if mesh.shape["hold"] == 64 else 2
    return nx, mesh.shape["hold"] // (2 * nz), nz


def solution(mesh):
    nx, ny, nz = sizes(mesh)
    split = Mesh(mesh.devices.reshape(nx, ny, nz, 2), AXES)
    rows = P(AXES, None)
    return jax.shard_map(
        functools.partial(body, nx, ny, nz),
        mesh=split,
        in_specs=(rows, P(AXES), P(AXES, None, None), P(AXES, None, None), P(AXES), P(AXES, None, None), P(AXES, None, None)),
        out_specs=(rows, rows),
        check_vma=False,
    )
```

```python
import functools
import math

import jax
import jax.numpy as jnp
from jax import lax
from jax.experimental import pallas as pl
from jax.experimental.pallas import tpu as pltpu
from jax.sharding import Mesh
from jax.sharding import PartitionSpec as P

HEADS = 32
KV_HEADS = 16
HEAD_DIM = 128
TYPES = 4
LOCAL = HEADS // TYPES
FIRST = LOCAL // 2
AXES = ("x", "y", "z", "c")
MESH = pl.DeviceIdType.MESH

SCALE2 = math.log2(math.e) / 168.0**0.5
LN2 = math.log(2.0)
MASKED = -1e30
FLOOR = -1e29

NT = (((1,), (1,)), ((), ()))
NN = (((1,), (0,)), ((), ()))


def kernel(
    flat_hbm, len_hbm, table_hbm, k_ref, v_ref, ks_ref, vs_ref,
    out_ref, log_ref,
    flat_ref, len_ref, table_ref, q_ref, own_len, zq, zl, turn, turn2, qg, kbuf, vbuf, pbuf, ksb, vsb,
    osend, msend, orecv, mrecv, osend2, msend2, orecv2, mrecv2, so, sm, sl, natural,
    small_sem, local_sem, kv_send, kv_recv, zq_send, zq_recv, zl_send, zl_recv,
    xy_send, xy_recv, ro_send, ro_recv, rm_send, rm_recv,
    fo_send, fo_recv, fm_send, fm_recv,
):
    nx, ny, nz = (lax.axis_size(a) for a in AXES[:3])
    x, y, z, c = (lax.axis_index(a) for a in AXES)
    rows = nz * 2
    mine, plane = z * 2 + c, x * ny + y
    other = 1 - c
    odd = lax.rem(z, 2)
    pairs = [z + 1 - 2 * odd, lax.rem(z + nz - 1 + 2 * odd, nz)]

    def kind(zz, cc):
        return lax.rem(zz, 2) * 2 + cc

    def columns(s, t, e):
        return pl.ds(pl.multiple_of((s * 8 + t * 2 + e) * HEAD_DIM, HEAD_DIM), HEAD_DIM)

    small = [
        pltpu.make_async_copy(src, dst, small_sem.at[i])
        for i, (src, dst) in enumerate([(flat_hbm, flat_ref), (len_hbm, len_ref), (table_hbm, table_ref)])
    ]
    for copy in small:
        copy.start()
    line = [(dz, dc) for dz in range(nz) for dc in range(2) if (dz, dc) != (0, 0)]
    line.sort(key=lambda d: -min(d[0], nz - d[0]))
    sheet = [(dx, dy) for dx in range(nx) for dy in range(ny) if (dx, dy) != (0, 0)]
    sheet.sort(key=lambda d: -min(d[0], nx - d[0]) - min(d[1], ny - d[1]))

    def line_id(dz, dc):
        return {"z": lax.rem(z + dz, nz), "c": lax.rem(c + dc, 2)}

    def sheet_id(dx, dy):
        return {"x": lax.rem(x + dx, nx), "y": lax.rem(y + dy, ny)}

    barrier = pltpu.get_barrier_semaphore()
    for dz, dc in line:
        pl.semaphore_signal(barrier, inc=1, device_id=line_id(dz, dc), device_id_type=MESH)
    for dx, dy in sheet:
        pl.semaphore_signal(barrier, inc=1, device_id=sheet_id(dx, dy), device_id_type=MESH)

    mykind = kind(z, c)
    loads = [
        pltpu.make_async_copy(ks_ref, ksb, local_sem.at[0]),
        pltpu.make_async_copy(vs_ref, vsb, local_sem.at[1]),
    ]
    own = []
    for e in range(2):
        copies = []
        for s in range(2):
            at, span = e * 4 + s * 2 + 2, columns(s, mykind, e)
            copies += [
                pltpu.make_async_copy(k_ref.at[:, :, span], kbuf.at[e, s, 0], local_sem.at[at]),
                pltpu.make_async_copy(v_ref.at[:, :, span], vbuf.at[e, s, 0], local_sem.at[at + 1]),
            ]
        own.append(copies)
        loads = loads + copies
    for load in loads:
        load.start()

    for copy in small:
        copy.wait()
    flat = flat_ref[...].astype(jnp.float32)
    for t in range(TYPES):
        for i in range(LOCAL):
            h = 16 * (i % 4 // 2) + 4 * t + 2 * (i // 4) + i % 2
            turn2[i, 0:1, :] = flat[:, h * HEAD_DIM : (h + 1) * HEAD_DIM]
        q_ref[t] = turn2[:, 0, :].astype(jnp.bfloat16)
    own_len[...] = jnp.full((1, 128), len_ref[0], jnp.int32).astype(jnp.float32)
    offset = lax.broadcasted_iota(jnp.int32, (1, 128), 1)
    for b in range(2):
        pbuf[0, b : b + 1, :] = (table_ref[b] * 128 + offset).astype(jnp.float32)

    pl.semaphore_wait(barrier, len(line) + len(sheet))

    def remote(src, dst, send, recv, device):
        return pltpu.make_async_remote_copy(
            src_ref=src, dst_ref=dst, send_sem=send, recv_sem=recv, device_id=device, device_id_type=MESH
        )

    def line_slot(dz, dc):
        return lax.rem(z + nz - dz, nz) * 2 + lax.rem(c + dc, 2)

    def line_gather(dz, dc, slot):
        i, to = dz * 2 + dc, kind(lax.rem(z + dz, nz), lax.rem(c + dc, 2))
        device = line_id(dz, dc)
        return [
            remote(q_ref.at[to], zq.at[slot], zq_send.at[i], zq_recv.at[i], device),
            remote(own_len, zl.at[slot], zl_send.at[i], zl_recv.at[i], device),
        ]

    for dz, dc in line:
        for copy in line_gather(dz, dc, mine):
            copy.start()
    partner = {"c": other}
    places = [remote(pbuf.at[0], pbuf.at[1], kv_send.at[24], kv_recv.at[24], partner)]
    for s in range(2):
        for dc in range(2):
            i, device = 2 * s + dc, {"z": pairs[s], "c": lax.rem(c + dc, 2)}
            places.append(remote(pbuf.at[0], pbuf.at[2 + i], kv_send.at[25 + i], kv_recv.at[25 + i], device))
    swaps = []
    for e in range(2):
        copies = []
        for ref, buf, at in ((k_ref, kbuf, e * 12), (v_ref, vbuf, e * 12 + 6)):
            for s in range(2):
                for dc in range(2):
                    i, core = at + 2 + 2 * s + dc, lax.rem(c + dc, 2)
                    source = ref.at[:, :, columns(s, kind(pairs[s], core), e)]
                    device = {"z": pairs[s], "c": core}
                    copies.append(remote(source, buf.at[e, s, 2 + dc], kv_send.at[i], kv_recv.at[i], device))
            for s in range(2):
                source = ref.at[:, :, columns(s, kind(z, other), e)]
                copies.append(remote(source, buf.at[e, s, 1], kv_send.at[at + s], kv_recv.at[at + s], partner))
        swaps.append(copies)
    for copy in places + swaps[0] + swaps[1]:
        copy.start()
    zq[pl.ds(mine, 1)] = q_ref[pl.ds(mykind, 1)]
    zl[pl.ds(mine, 1)] = own_len[...][None]

    loads[0].wait()
    loads[1].wait()
    query = q_ref[...].astype(jnp.float32).reshape(HEADS, HEAD_DIM)
    place = lax.broadcasted_iota(jnp.int32, (HEADS, HEAD_DIM), 0)
    head_kv = place % 4 // 2 * 8 + place // LOCAL * 2 + place % LOCAL // 4
    own_scores = jnp.zeros((HEADS, 128), jnp.float32)
    for kv in range(KV_HEADS):
        picked = jnp.where(head_kv == kv, query, 0.0).astype(jnp.bfloat16)
        own_scores += lax.dot_general(
            picked, ksb[0, :, kv * HEAD_DIM : (kv + 1) * HEAD_DIM], NT, preferred_element_type=jnp.float32
        )
    own_scores = own_scores * SCALE2
    own_max = jnp.max(own_scores, axis=1, keepdims=True)
    own_weights = jnp.exp2(own_scores - own_max).astype(jnp.bfloat16)
    own_sum = jnp.sum(own_weights.astype(jnp.float32), axis=1, keepdims=True)
    own_out = jnp.zeros((HEADS, HEAD_DIM), jnp.float32)
    for kv in range(KV_HEADS):
        part = lax.dot_general(
            own_weights, vsb[0, :, kv * HEAD_DIM : (kv + 1) * HEAD_DIM], NN, preferred_element_type=jnp.float32
        )
        own_out += jnp.where(head_kv == kv, part, 0.0)
    so[...] = own_out
    sm[...] = jnp.broadcast_to(own_max, (HEADS, 128))
    sl[...] = jnp.broadcast_to(own_sum, (HEADS, 128))

    for dz, dc in line:
        for copy in line_gather(dz, dc, line_slot(dz, dc)):
            copy.wait_recv()
    turn[...] = zq[...].astype(jnp.float32)
    for h in range(LOCAL):
        qg[pl.ds(plane, 1), h] = turn[:, h, :].astype(jnp.bfloat16)[None]
    length = zl[:, 0, :]
    high = jnp.floor(length * (1.0 / 256.0))
    lane = lax.broadcasted_iota(jnp.int32, (rows, 128), 1)
    qg[pl.ds(plane, 1), LOCAL] = jnp.where(lane < 64, high, length - high * 256.0).astype(jnp.bfloat16)[None]

    def sheet_pass(colour, bx, by, dx, dy):
        tiles = pl.ds(0, FIRST) if colour == 0 else pl.ds(FIRST, LOCAL + 1 - FIRST)
        block = lax.rem(x + bx, nx) * ny + lax.rem(y + by, ny)
        seen = lax.rem(bx + nx - dx, nx) * ny + lax.rem(by + ny - dy, ny)
        sent = (bx + dx) * ny + dy if colour == 0 else dx * ny + by + dy
        return remote(
            qg.at[block, tiles], qg.at[block, tiles],
            xy_send.at[colour, sent], xy_recv.at[colour, seen], sheet_id(dx, dy),
        )

    def sheet_arrival(colour, bx, by):
        tiles = pl.ds(0, FIRST) if colour == 0 else pl.ds(FIRST, LOCAL + 1 - FIRST)
        block = qg.at[lax.rem(x + bx, nx) * ny + lax.rem(y + by, ny), tiles]
        i = bx * ny + by
        return remote(block, block, xy_send.at[colour, i], xy_recv.at[colour, i], sheet_id(0, 0))

    along_x = [1 + (i // 2 if i % 2 == 0 else nx - 2 - i // 2) for i in range(nx - 1)]
    along_y = [1 + (i // 2 if i % 2 == 0 else ny - 2 - i // 2) for i in range(ny - 1)]
    near_first = along_x + along_y
    along_x.sort(key=lambda d: -min(d, nx - d))
    along_y.sort(key=lambda d: -min(d, ny - d))
    passes = [(0, 0, 0, dx, 0) for dx in along_x] + [(1, 0, 0, 0, dy) for dy in along_y]
    passes += [(0, 0, 0, 0, dy) for dy in along_y] + [(1, 0, 0, dx, 0) for dx in along_x]
    for step in passes:
        sheet_pass(*step).start()
    seen_first = [(0, bx, 0) for bx in along_x] + [(1, 0, by) for by in along_y]
    for colour, bx, by in sorted(seen_first, key=lambda b: near_first.index(b[1] + b[2])):
        sheet_arrival(colour, bx, by).wait_recv()
        onward = [(0, bx, 0, 0, dy) for dy in along_y] if colour == 0 else [(1, 0, by, dx, 0) for dx in along_x]
        for step in onward:
            sheet_pass(*step).start()
        passes += onward

    for copy in places:
        copy.wait_recv()
    tokens = 8 * 128
    positions = [
        jnp.concatenate([pbuf[p, b : b + 1, :] for p in (0, 1, 2 + 2 * s, 3 + 2 * s) for b in range(2)], axis=1)
        for s in range(2)
    ]
    ones = jnp.ones((tokens, HEAD_DIM), jnp.bfloat16)
    group = ny * 2 * rows
    pile = min(rows, 8)

    def packed(tile):
        tile = tile.reshape(-1, pile, 128)
        line = sum(pltpu.roll(tile[i], 64 * i, 1, stride=8, stride_axis=0) for i in range(rows // pile))
        return jnp.sum(line, axis=0, keepdims=True)

    def sheet_return(e, i, device, here, there):
        return [
            remote(osend.at[e, here], orecv.at[e, there], ro_send.at[e, i], ro_recv.at[e, i], device),
            remote(msend.at[e, here], mrecv.at[e, there], rm_send.at[e, i], rm_recv.at[e, i], device),
        ]

    def chunk(e, k):
        column = lax.rem(x + k, nx)
        base = column * ny
        if e == 0:
            for dy in range(1, ny):
                sheet_arrival(0, k, dy).wait_recv()

            def arrive():
                for dy in range(ny):
                    sheet_arrival(1, k, dy).wait_recv()

            pl.when(k > 0)(arrive)
        tile = qg[pl.ds(base, ny), LOCAL].astype(jnp.float32)
        wide = tile[:, :, 0:1] * 256.0 + tile[:, :, 64:65]
        limit = jnp.broadcast_to(wide[:, None], (ny, 2, rows, 1)).reshape(group, 1)
        lanes = lax.broadcasted_iota(jnp.int32, (ny, rows, 128), 2)
        stats = jnp.zeros((ny, rows, 128), jnp.float32)
        for s in range(2):
            g = 2 * e + s
            queries = qg[pl.ds(base, ny), 2 * g : 2 * g + 2].reshape(group, HEAD_DIM)
            keys = kbuf[e, s].reshape(tokens, HEAD_DIM)
            values = vbuf[e, s].reshape(tokens, HEAD_DIM)
            scores = lax.dot_general(queries, keys, NT, preferred_element_type=jnp.float32) * SCALE2
            scores = jnp.where(positions[s] < limit, scores, MASKED)
            top = jnp.maximum(jnp.max(scores, axis=1, keepdims=True), FLOOR)
            weights = jnp.exp2(scores - top).astype(jnp.bfloat16)
            both = lax.dot_general(
                weights, jnp.concatenate([values, ones], axis=1), NN, preferred_element_type=jnp.float32
            )
            osend[e, pl.ds(base, ny), 2 * s : 2 * s + 2] = (
                both[:, :HEAD_DIM].astype(jnp.bfloat16).reshape(ny, 2, rows, HEAD_DIM)
            )
            tops = jnp.broadcast_to(top, (group, 128)).reshape(ny, 2, rows, 128)
            sums = both[:, HEAD_DIM:].reshape(ny, 2, rows, 128)
            for j in range(2):
                stats = jnp.where(lanes == 2 * s + j, tops[:, j], stats)
                stats = jnp.where(lanes == 4 + 2 * s + j, sums[:, j], stats)
        for i in range(ny):
            msend[e, pl.ds(base + i, 1)] = packed(stats[i])[None]
        for dy in sorted(range(ny), key=lambda d: -min(d, ny - d)):
            row = lax.rem(y + dy, ny)
            there = column * ny + row

            def leave(dy=dy, row=row, there=there):
                for copy in sheet_return(e, k * ny + dy, {"x": column, "y": row}, there, plane):
                    copy.start()

            if dy == 0:
                pl.when(k > 0)(leave)
            else:
                leave()

    for e in range(2):
        for copy in own[e]:
            copy.wait()
        for copy in swaps[e]:
            copy.wait_recv()
        lax.fori_loop(0, nx, lambda k, carry, e=e: (chunk(e, lax.rem(k + e, nx)), carry)[1], 0)
        orecv[e, pl.ds(plane, 1)] = osend[e, pl.ds(plane, 1)]
        mrecv[e, pl.ds(plane, 1)] = msend[e, pl.ds(plane, 1)]

    def line_return(e, dz, dc, here, there):
        i = dz * 2 + dc
        device = line_id(dz, dc)
        return [
            remote(osend2.at[e, here], orecv2.at[e, there], fo_send.at[e, i], fo_recv.at[e, i], device),
            remote(msend2.at[e], mrecv2.at[e, there], fm_send.at[e, i], fm_recv.at[e, i], device),
        ]

    count = nx * ny
    at_row = lax.broadcasted_iota(jnp.int32, (rows, 128), 0) * 8
    zero = jnp.zeros((rows, HEAD_DIM), jnp.float32)
    for e in range(2):
        for dx, dy in sheet:
            slot = lax.rem(x + nx - dx, nx) * ny + lax.rem(y + ny - dy, ny)
            for copy in sheet_return(e, dx * ny + dy, sheet_id(dx, dy), slot, slot):
                copy.wait_recv()
        best = jnp.max(mrecv[e], axis=0)

        def merge(s, carry, e=e, best=best):
            total, out = carry
            part = mrecv[e, pl.ds(s, 1)][0]
            factor = jnp.exp2(part - best)
            total = total + pltpu.roll(factor, 4, 1) * part
            spread = jnp.broadcast_to(factor, (rows, 128))
            block = orecv[e, pl.ds(s, 1)][0].astype(jnp.float32)
            out = tuple(
                out[h] + jnp.sum(jnp.where(lane == at_row + h, spread, 0.0), axis=1, keepdims=True) * block[h]
                for h in range(4)
            )
            return total, out

        total, out = lax.fori_loop(0, count, merge, (jnp.zeros_like(best), (zero,) * 4), unroll=4)
        msend2[e] = jnp.where(lane[:1] % 8 < 4, best, total)
        for h in range(4):
            turn2[4 * e + h] = out[h]
        for r in range(rows):
            osend2[e, r] = turn2[4 * e : 4 * e + 4, r, :]
        for dz, dc in line:
            target = lax.rem(z + dz, nz) * 2 + lax.rem(c + dc, 2)
            for copy in line_return(e, dz, dc, target, mine):
                copy.start()
        orecv2[e, pl.ds(mine, 1)] = osend2[e, pl.ds(mine, 1)]
        mrecv2[e, pl.ds(mine, 1)] = msend2[e][None]

    for copy in places + swaps[0] + swaps[1]:
        copy.wait_send()
    for step in passes:
        sheet_pass(*step).wait_send()
    for dz, dc in line:
        target = lax.rem(z + dz, nz) * 2 + lax.rem(c + dc, 2)
        for copy in line_gather(dz, dc, mine):
            copy.wait_send()
        for e in range(2):
            for copy in line_return(e, dz, dc, target, mine):
                copy.wait_send()
    for dx, dy in sheet:
        i, device = dx * ny + dy, sheet_id(dx, dy)
        there = lax.rem(x + dx, nx) * ny + lax.rem(y + dy, ny)
        for e in range(2):
            for copy in sheet_return(e, i, device, there, plane):
                copy.wait_send()

    lane_of = lax.broadcasted_iota(jnp.int32, (4, 128), 1)
    line_log = jnp.zeros((1, 128), jnp.float32)
    head_row = lax.broadcasted_iota(jnp.int32, (4, 128), 0)
    pick = mine * 8 + lax.broadcasted_iota(jnp.int32, (4, 128), 0)
    for e in range(2):
        for dz, dc in line:
            slot = line_slot(dz, dc)
            for copy in line_return(e, dz, dc, slot, slot):
                copy.wait_recv()
        for t in range(TYPES):
            heads = slice(t * LOCAL + 4 * e, t * LOCAL + 4 * e + 4)
            slots = [zz * 2 + t % 2 for zz in range(nz) if zz % 2 == t // 2]
            tops, sums = [sm[heads, 0:1]], [sl[heads, 0:1]]
            for slot in slots:
                row = jnp.broadcast_to(mrecv2[e, slot], (4, 128))
                tops.append(jnp.sum(jnp.where(lane_of == pick, row, 0.0), axis=1, keepdims=True))
                sums.append(jnp.sum(jnp.where(lane_of == pick + 4, row, 0.0), axis=1, keepdims=True))
            top = functools.reduce(jnp.maximum, tops)
            factors = [jnp.exp2(m - top) for m in tops]
            normalizer = sum(f * l for f, l in zip(factors, sums))
            numerator = factors[0] * so[heads, :]
            for f, slot in zip(factors[1:], slots):
                numerator += f * orecv2[e, slot]
            numerator = numerator / normalizer
            logs = jnp.broadcast_to(top * LN2 + jnp.log(normalizer), (4, 128))
            wanted = 16 * (head_row // 2) + 4 * t + 2 * e + head_row % 2
            line_log += jnp.sum(jnp.where(lane_of == wanted, logs, 0.0), axis=0, keepdims=True)
            for s in range(2):
                first = 16 * s + 4 * t + 2 * e
                natural[first : first + 2, :] = numerator[2 * s : 2 * s + 2]
    for h in range(HEADS):
        out_ref[:, h * HEAD_DIM : (h + 1) * HEAD_DIM] = natural[h : h + 1, :].astype(jnp.bfloat16)
    log_ref[...] = line_log[:, :HEADS]


def settle(out_ref, log_ref, out_final, log_final):
    out_final[...] = out_ref[...]
    log_final[...] = log_ref[...]


def body(nx, ny, nz, queries, prefix_len, prefix_keys, prefix_values, block_table, suffix_keys, suffix_values):
    rows, count = nz * 2, nx * ny
    vmem, hbm = pl.BlockSpec(memory_space=pltpu.VMEM), pl.BlockSpec(memory_space=pltpu.HBM)
    bf16, f32 = jnp.bfloat16, jnp.float32
    dma = pltpu.SemaphoreType.DMA
    out, logs = pl.pallas_call(
        kernel,
        name="decode",
        out_shape=[
            pltpu.VMEM((1, HEADS * HEAD_DIM), bf16),
            pltpu.VMEM((1, HEADS), f32),
        ],
        in_specs=[hbm, hbm, hbm, hbm, hbm, hbm, hbm],
        out_specs=[vmem, vmem],
        scratch_shapes=[
            pltpu.VMEM((1, HEADS * HEAD_DIM), bf16),
            pltpu.SMEM((1,), jnp.int32),
            pltpu.SMEM((2,), jnp.int32),
            pltpu.VMEM((TYPES, LOCAL, HEAD_DIM), bf16),
            pltpu.VMEM((1, 128), f32),
            pltpu.VMEM((rows, LOCAL, HEAD_DIM), bf16),
            pltpu.VMEM((rows, 1, 128), f32),
            pltpu.VMEM((rows, LOCAL, HEAD_DIM), f32),
            pltpu.VMEM((LOCAL, rows, HEAD_DIM), f32),
            pltpu.VMEM((count, LOCAL + 1, rows, HEAD_DIM), bf16),
            pltpu.VMEM((2, 2, 4, 2, 128, HEAD_DIM), bf16),
            pltpu.VMEM((2, 2, 4, 2, 128, HEAD_DIM), bf16),
            pltpu.VMEM((6, 8, 128), f32),
            pltpu.VMEM((1, 128, KV_HEADS * HEAD_DIM), bf16),
            pltpu.VMEM((1, 128, KV_HEADS * HEAD_DIM), bf16),
            pltpu.VMEM((2, count, 4, rows, HEAD_DIM), bf16),
            pltpu.VMEM((2, count, 1, 128), f32),
            pltpu.VMEM((2, count, 4, rows, HEAD_DIM), bf16),
            pltpu.VMEM((2, count, 1, 128), f32),
            pltpu.VMEM((2, rows, 4, HEAD_DIM), f32),
            pltpu.VMEM((2, 1, 128), f32),
            pltpu.VMEM((2, rows, 4, HEAD_DIM), f32),
            pltpu.VMEM((2, rows, 1, 128), f32),
            pltpu.VMEM((HEADS, HEAD_DIM), f32),
            pltpu.VMEM((HEADS, 128), f32),
            pltpu.VMEM((HEADS, 128), f32),
            pltpu.VMEM((HEADS, HEAD_DIM), f32),
            dma((3,)), dma((10,)), dma((29,)), dma((29,)),
            dma((rows,)), dma((rows,)), dma((rows,)), dma((rows,)),
            dma((2, count)), dma((2, count)),
            dma((2, count)), dma((2, count)), dma((2, count)), dma((2, count)),
            dma((2, rows)), dma((2, rows)), dma((2, rows)), dma((2, rows)),
        ],
        compiler_params=pltpu.CompilerParams(
            collective_id=0, has_side_effects=True, vmem_limit_bytes=63 * 1024 * 1024
        ),
    )(queries, prefix_len, block_table, prefix_keys, prefix_values, suffix_keys, suffix_values)
    return tuple(pl.pallas_call(
        settle,
        name="settle",
        out_shape=[jax.ShapeDtypeStruct(out.shape, bf16), jax.ShapeDtypeStruct(logs.shape, f32)],
        in_specs=[vmem, vmem],
        out_specs=[vmem, vmem],
    )(*(pltpu.with_memory_space_constraint(a, pltpu.VMEM) for a in (out, logs))))


def sizes(mesh):
    nx = mesh.shape["grp"]
    nz = 8 if mesh.shape["hold"] == 64 else 2
    return nx, mesh.shape["hold"] // (2 * nz), nz


def solution(mesh):
    nx, ny, nz = sizes(mesh)
    split = Mesh(mesh.devices.reshape(nx, ny, nz, 2), AXES)
    rows = P(AXES, None)
    return jax.shard_map(
        functools.partial(body, nx, ny, nz),
        mesh=split,
        in_specs=(rows, P(AXES), P(AXES, None, None), P(AXES, None, None), P(AXES), P(AXES, None, None), P(AXES, None, None)),
        out_specs=(rows, rows),
        check_vma=False,
    )
```
